128 devices in a mesh: ens: 64 (over z, y, x_hi, core), batch: 2 (over x_lo).
Axes of the slice: x: 4 (x_hi: 2, x_lo: 2; x = x_hi * 2 + x_lo), y: 4, z: 4, core: 2. Of those that a mesh axis runs over, the one named last changes fastest.
Arguments:
- replay_obs: bfloat16 [512, 1024], P('batch'), may hold values from -4.1875 to 4.1875
- replay_next: bfloat16 [512, 1024], P('batch'), may hold values from -4.1875 to 4.1875
- batch_rows: int32 [64], P('batch'), may hold values from 0 to 255
- data_action: int32 [64], P('batch'), may hold values from 0 to 255
- next_action: int32 [64], P('batch'), may hold values from 0 to 255
- sampled_actions: int32 [64, 16], P('batch'), may hold values from 0 to 255
- reward: float32 [64], P('batch'), may hold values from -6 to 6
- next_logp: float32 [64], P('batch'), may hold values from -6 to 2
- action_table: bfloat16 [256, 1024], replicated, may hold values from -4.1875 to 4.1875
- w1: bfloat16 [64, 4096, 1024], P('ens'), may hold values from -0.1875 to 0.1875
- w2: float32 [64, 4096], P('ens'), may hold values from -0.375 to 0.375
Outputs:
- grad_w1: float32 [64, 4096, 1024], P('ens', 'batch')
- grad_w2: float32 [64, 4096], P('ens')
- critic_stats: float32 [64, 3], P('ens')
The draws below stay inside these ranges and needn't reach their ends.
Inputs may be any that keep to these rules, and one draw needn't show every extreme that they name: `batch_rows`: each entry is a row of the own block of 256 replay rows that holds its state.
All inputs are finite; a program needn't handle non-finite values.
Results may differ from the reference program's by a relative error of at most 0.0045.
Values may be sent and summed in bfloat16 or wider, within the bound.
A program may use at most 128 MiB of HBM per device.

```python
import jax
import jax.numpy as jnp
from jax import lax

D = 1024
H = 4096
NACT = 256
A = 16
S_DEV = 32
BUF_DEV = 256
ENS = 64
STATES = 64
N_BATCH = 2


def touch_ends(array, key, least, high):
    index_at = [jax.random.randint(jax.random.fold_in(key, axis), (), 0, length) for axis, length in enumerate(array.shape)]
    longest = array.shape.index(max(array.shape))
    next_to = index_at[:longest] + [(index_at[longest] + 1) % array.shape[longest]] + index_at[longest + 1:]
    return array.at[tuple(index_at)].set(least).at[tuple(next_to)].set(high)


def shard_levels(own_key, shape, shards, least, top_value):
    factor_of, own = 1.0, jax.random.fold_in(own_key, 6)
    for axis_at, shards_of in shards:
        steps = jnp.exp(jax.random.uniform(jax.random.fold_in(own, axis_at), (shards_of,), jnp.float32, least / len(shards), top_value / len(shards)))
        factor_of = factor_of * jnp.repeat(steps, shape[axis_at] // shards_of).reshape([-1 if axis == axis_at else 1 for axis in range(len(shape))])
    return factor_of


def scatter_about(stream_key, extent, deviation, bound, pieces=(), kind=jnp.bfloat16):
    array = jax.random.normal(stream_key, extent, jnp.float32) * deviation
    if len(pieces) > 0:
        array = shard_levels(stream_key, extent, pieces, -0.22, 0.18) * array
    return jnp.clip(array, min=-bound, max=bound).astype(kind)


def setup_inputs(seed: int = 0) -> dict:
    key_list = jax.random.split(jax.random.key(seed), 12)
    return {
        "replay_obs": scatter_about(key_list[0], (N_BATCH * BUF_DEV, D), 0.7, 4.1875, ((0, 2),)),
        "replay_next": scatter_about(key_list[1], (N_BATCH * BUF_DEV, D), 0.7, 4.1875, ((0, 2),)),
        "batch_rows": touch_ends(jax.random.randint(key_list[2], (STATES,), 0, BUF_DEV), jax.random.fold_in(key_list[2], 1), 0, BUF_DEV - 1).astype(jnp.int32),
        "data_action": touch_ends(jax.random.randint(key_list[3], (STATES,), 0, NACT), jax.random.fold_in(key_list[3], 1), 0, NACT - 1).astype(jnp.int32),
        "next_action": touch_ends(jax.random.randint(key_list[4], (STATES,), 0, NACT), jax.random.fold_in(key_list[4], 1), 0, NACT - 1).astype(jnp.int32),
        "sampled_actions": touch_ends(jax.random.randint(key_list[5], (STATES, A), 0, NACT), jax.random.fold_in(key_list[5], 1), 0, NACT - 1).astype(jnp.int32),
        "reward": scatter_about(key_list[6], (STATES,), 1.0, 6.0, ((0, 2),), jnp.float32),
        "next_logp": jnp.clip(-6.0 + 8.0 * jax.random.uniform(key_list[7], (STATES,), jnp.float32) ** shard_levels(key_list[7], (STATES,), ((0, 2),), -0.2, 0.2), -6.0, 2.0),
        "action_table": scatter_about(key_list[8], (NACT, D), 0.7, 4.1875),
        "w1": scatter_about(key_list[9], (ENS, H, D), D ** -0.5, 0.1875, ((0, 64),)),
        "w2": scatter_about(key_list[10], (ENS, H), (4.0 / H ** 0.5), 0.375, ((0, 64),), jnp.float32),
    }


discount = 0.99
entropy_temp = 0.2
penalty_weight = 1.0
diversity_weight = 1000.0

def silu_terms(preact):
    sigmoid_v = jax.nn.sigmoid(preact)
    silu_out = preact * sigmoid_v
    slope_one = sigmoid_v * (1.0 + preact * (1.0 - sigmoid_v))
    return (silu_out, slope_one, sigmoid_v)

def reference(replay_obs, replay_next, batch_rows, data_action, next_action, sampled_actions, reward, next_logp, action_table, w1, w2):
    owners = jnp.arange(STATES, dtype=jnp.int32) // S_DEV
    row_ids = owners * BUF_DEV + batch_rows.astype(jnp.int32)
    obs_rows = jnp.take(replay_obs, row_ids, axis=0).astype(jnp.float32)
    next_rows = jnp.take(replay_next, row_ids, axis=0).astype(jnp.float32)
    table_f = action_table.astype(jnp.float32)
    x_next = (next_rows + jnp.take(table_f, next_action, axis=0)).astype(jnp.bfloat16)
    x_data = (obs_rows + jnp.take(table_f, data_action, axis=0)).astype(jnp.bfloat16)
    x_samp = (obs_rows[:, None, :] + jnp.take(table_f, sampled_actions, axis=0)).astype(jnp.bfloat16)
    x_samp = x_samp.reshape(STATES * A, D)

    def data_pass(weight, readout):
        preact = jnp.dot(x_data, weight.T, preferred_element_type=jnp.float32)
        silu_out, slope_one, sigmoid_v = silu_terms(preact)
        coeffs = (readout * slope_one).astype(jnp.bfloat16)
        grad_in = jnp.dot(coeffs, weight, preferred_element_type=jnp.float32)
        in_norm = jnp.sqrt(lax.optimization_barrier(jnp.sum(grad_in * grad_in, axis=-1, keepdims=True)) + 1.0)
        return (preact, silu_out, slope_one, sigmoid_v, coeffs, in_norm, grad_in / in_norm)

    def forward(params):
        weight, readout = params
        pre_next = jnp.dot(x_next, weight.T, preferred_element_type=jnp.float32)
        q_next = lax.optimization_barrier(jnp.sum(silu_terms(pre_next)[0] * readout, axis=-1))
        unit_dir = data_pass(weight, readout)[6]
        return (q_next, unit_dir)
    q_next_all, units = lax.map(forward, (w1, w2))
    target_floor = lax.optimization_barrier(jnp.min(q_next_all, axis=0))
    target = reward + discount * (target_floor - entropy_temp * next_logp)
    spread = lax.optimization_barrier(jnp.sum(units, axis=0))

    def backward(params):
        weight, readout = params
        preact, silu_out, slope_one, sigmoid_v, coeffs, in_norm, unit_dir = data_pass(weight, readout)
        q_data = lax.optimization_barrier(jnp.sum(silu_out * readout, axis=-1))
        pre_samp = jnp.dot(x_samp, weight.T, preferred_element_type=jnp.float32)
        silu_samp, slope_samp, _ = silu_terms(pre_samp)
        q_samp = lax.optimization_barrier(jnp.sum(silu_samp * readout, axis=-1)).reshape(STATES, A)
        td_gap = q_data - target
        log_mass = jnp.log(lax.optimization_barrier(jnp.sum(jnp.exp(q_samp), axis=-1)))
        action_prob = jnp.exp(q_samp - log_mass[:, None])
        div_row = lax.optimization_barrier(jnp.sum(unit_dir * (spread - unit_dir), axis=-1))
        stats = jnp.stack([jnp.sum(td_gap * td_gap), jnp.sum(log_mass - q_data), jnp.sum(div_row)]) / STATES
        dq_data = (2.0 * td_gap - penalty_weight) / STATES
        dq_samp = (penalty_weight * action_prob / STATES).reshape(STATES * A)
        dunit = 2.0 * diversity_weight / (ENS - 1) / STATES * (spread - unit_dir)
        dgrad = ((dunit - unit_dir * lax.optimization_barrier(jnp.sum(unit_dir * dunit, axis=-1, keepdims=True))) / in_norm).astype(jnp.bfloat16)
        dcoef = jnp.dot(dgrad, weight.T, preferred_element_type=jnp.float32)
        curve_two = sigmoid_v * (1.0 - sigmoid_v) * (2.0 + preact * (1.0 - 2.0 * sigmoid_v))
        dpre_data = (dq_data[:, None] * readout * slope_one + dcoef * readout * curve_two).astype(jnp.bfloat16)
        dpre_samp = (dq_samp[:, None] * readout * slope_samp).astype(jnp.bfloat16)
        grad_v = lax.optimization_barrier(jnp.sum(dq_data[:, None] * silu_out, axis=0)) + lax.optimization_barrier(jnp.sum(dq_samp[:, None] * silu_samp, axis=0)) + lax.optimization_barrier(jnp.sum(dcoef * slope_one, axis=0))
        grad_w = jnp.dot(dpre_data.T, x_data, preferred_element_type=jnp.float32)
        grad_w = grad_w + jnp.dot(dpre_samp.T, x_samp, preferred_element_type=jnp.float32)
        grad_w = grad_w + jnp.dot(coeffs.T, dgrad, preferred_element_type=jnp.float32)
        return (grad_w, grad_v, stats)
    grad_w1, grad_w2, critic_stats = lax.map(backward, (w1, w2))
    return (grad_w1, grad_w2, critic_stats)
```

```python
import jax
import jax.numpy as jnp
from jax import lax
from jax.experimental import pallas as pl
from jax.experimental.pallas import tpu as pltpu
from jax.sharding import Mesh
from jax.sharding import PartitionSpec as P

ENS = ("ens_0", "ens_1", "ens_2", "ens_3")
MESH_ID = pl.DeviceIdType.MESH
f32, bf16 = jnp.float32, jnp.bfloat16

D, H, HH = 1024, 4096, 2048
S, A, NACT = 32, 16, 256
ROWS = S * A
CH = 512
NCH = H // CH
TILE = 256
SUB = 32
PLANE = 32
COUNT = 64
discount, entropy_temp, penalty_weight, diversity_weight = 0.99, 0.2, 1.0, 1000.0

NN = (((1,), (0,)), ((), ()))
NT = (((1,), (1,)), ((), ()))
TN = (((0,), (0,)), ((), ()))


def dot(a, b, dims=NN):
    return lax.dot_general(a, b, dims, preferred_element_type=f32)


def mo(x, m):
    return pl.multiple_of(x, m)


def each(lo, hi, fn):
    def step(k, carry):
        fn(k)
        return carry

    lax.fori_loop(lo, hi, step, 0)


def iota(shape, dim):
    return lax.broadcasted_iota(jnp.int32, shape, dim)


def row8(x):
    return jnp.broadcast_to(x, (8, 128))


def main_kernel(
    obs_hbm, next_hbm, rows_hbm, dact_hbm, nact_hbm, sact_hbm, rew_hbm, logp_hbm, table_hbm, w_hbm, v_hbm,
    lhs_s, lhs_t, rhs_s, rhs_t, gw2_out, stats_out,
    tab_obs, tab_next, table, w, v, ids, sact, rl,
    xdn, xs, xd, tx_obs, rx_obs, tx_small, rx_small,
    vcol, gin, rx_g, tx_q, rx_q, units, rs_buf, q_buf, xr, xq, ag_tx, spread,
    h_buf, sl, silu, hd, q_sc, rx_qs, x_out, lt, rt, gw_part, gw2, stats_sc,
    in_sem, w_sem, out_sem, pair_s, pair_r, rs_s, rs_r, qs_s, qs_r, x_s, x_r, xq_s, xq_r, ag_s, ag_r,
):
    z, y, xh, core = (lax.axis_index(n) for n in ENS)
    b = lax.axis_index("batch")
    me = z * 8 + y * 2 + core
    xpos = xh * 2 + b

    def plane(k):
        j = lax.rem(me + k, PLANE)
        return j, (lax.div(j, 8), lax.rem(lax.div(j, 2), 4), xh, lax.rem(j, 2), b)

    def line(d):
        p = lax.rem(xpos + d, 4)
        return (z, y, lax.div(p, 2), core, lax.rem(p, 2))

    def tile_at(j):
        return pl.ds(mo(lax.div(j, 8) * 8, 8), 8), pl.ds(mo(lax.rem(j, 8) * 128, 128), 128)

    partner = (z, y, xh, core, 1 - b)
    h0 = mo(b * HH, HH)

    def far(src, dst, ssem, rsem, device):
        return pltpu.make_async_remote_copy(
            src_ref=src, dst_ref=dst, send_sem=ssem, recv_sem=rsem, device_id=device, device_id_type=MESH_ID
        )

    loads = [
        pltpu.make_async_copy(src, dst, in_sem.at[i])
        for i, (src, dst) in enumerate(
            [
                (rows_hbm, ids.at[0]), (dact_hbm, ids.at[1]), (nact_hbm, ids.at[2]), (sact_hbm, sact),
                (rew_hbm, rl.at[0]), (logp_hbm, rl.at[1]),
                (obs_hbm, tab_obs), (next_hbm, tab_next), (table_hbm, table), (v_hbm, v),
            ]
        )
    ]
    for c in loads:
        c.start()

    def w_copy(c):
        at = pl.ds(mo(c * CH, CH), CH)
        return pltpu.make_async_copy(w_hbm.at[at], w.at[at], w_sem.at[c])

    each(0, NCH, lambda c: w_copy(c).start())

    barrier = pltpu.get_barrier_semaphore()

    def greet(device):
        pl.semaphore_signal(barrier, inc=1, device_id=device, device_id_type=MESH_ID)

    each(1, PLANE, lambda k: greet(plane(k)[1]))
    for d in (1, 2, 3):
        greet(line(d))

    for c in loads:
        c.wait()

    lanes = iota((S, NACT), 1).astype(f32)
    eye = iota((S, S), 0) == iota((S, S), 1)
    ones = jnp.ones((S, NACT), bf16)

    def one_hot(i):
        diag = jnp.where(eye, jnp.broadcast_to(ids[i].astype(f32), (S, S)), 0.0).astype(bf16)
        return jnp.where(dot(diag, ones) == lanes, 1.0, 0.0).astype(bf16)

    def halved(x):
        return (x.astype(bf16).astype(f32) * 0.5).astype(bf16)

    own_oh = one_hot(0)
    obs = dot(own_oh, tab_obs[...])
    nxt = dot(own_oh, tab_next[...])
    tx_obs[...] = obs.astype(bf16)
    half_data = halved(obs + dot(one_hot(1), table[...]))
    xdn[0:S, :] = half_data
    xdn[S : 2 * S, :] = halved(nxt + dot(one_hot(2), table[...]))
    xd[0:S, :] = half_data
    tx_small[...] = jnp.zeros_like(tx_small)
    tx_small[0:A, 0:S] = sact[...].astype(f32)
    tx_small[A : A + 1, 0:S] = ids[1].astype(f32)
    tx_small[A + 1 : A + 2, 0:S] = rl[0]
    tx_small[A + 2 : A + 3, 0:S] = rl[1]

    def spread_v(i):
        at = pl.ds(mo(i * 128, 128), 128)
        vcol[at, :] = jnp.transpose(jnp.broadcast_to(v[:, at], (128, 128)))

    each(0, H // 128, spread_v)
    gin[...] = jnp.zeros_like(gin)

    def own_chunk(c, q_acc):
        w_copy(c).wait()
        at = pl.ds(mo(c * CH, CH), CH)
        wc = w[at, :]
        h = dot(wc, xdn[...], NT)
        th = jnp.tanh(h)
        a = h * th
        vc = vcol[at, 0 : 2 * S]
        q_acc = q_acc + jnp.sum((h + a) * vc, axis=0, keepdims=True)
        co = (0.5 * vc * ((1.0 + th) + (h - a * th))).astype(bf16)
        gin[...] += dot(co[:, 0:S], wc, TN)
        return q_acc

    q_own = lax.fori_loop(0, NCH // 2, own_chunk, jnp.zeros((1, 2 * S), f32))
    pl.semaphore_wait(barrier, PLANE - 1 + 3)
    cp_obs = far(tx_obs, rx_obs, pair_s.at[0], pair_r.at[0], partner)
    cp_small = far(tx_small, rx_small, pair_s.at[1], pair_r.at[1], partner)
    cp_obs.start()
    cp_small.start()
    q_own = lax.fori_loop(NCH // 2, NCH, own_chunk, q_own)

    tx_q[...] = jnp.zeros_like(tx_q)
    tx_q[:, 0 : 2 * S] = q_own

    def norm_of(g):
        return jnp.sqrt(jnp.sum(g * g, axis=-1, keepdims=True) + 1.0)

    g_own = gin[...]
    norm_own = norm_of(g_own)
    units[0:S, :] = g_own / norm_own

    def rs_copy(k):
        j, device = plane(k)
        r, c = tile_at(j)
        return far(units.at[r, c], rs_buf.at[k], rs_s.at[k], rs_r.at[k], device)

    def qs_copy(k):
        return far(tx_q, q_buf.at[k], qs_s.at[k], qs_r.at[k], plane(k)[1])

    each(1, PLANE, lambda k: rs_copy(k).start())
    each(1, PLANE, lambda k: qs_copy(k).start())
    cp_g = far(gin, rx_g, pair_s.at[2], pair_r.at[2], partner)
    cp_q = far(tx_q, rx_q, pair_s.at[3], pair_r.at[3], partner)
    cp_g.start()
    cp_q.start()

    def build(sact_f, base, off):
        row = iota((ROWS, S), 0)
        pick = jnp.where((row & (S - 1)) == iota((ROWS, S), 1), 1.0, 0.0).astype(bf16)
        each_sample = dot(pick, sact_f.astype(bf16), NT)
        mine = lax.shift_right_logical(iota((ROWS, A), 0), 5) == iota((ROWS, A), 1)
        index = dot(jnp.where(mine, each_sample, 0.0).astype(bf16), jnp.ones((A, NACT), bf16))
        oh = jnp.where(index == iota((ROWS, NACT), 1).astype(f32), 1.0, 0.0).astype(bf16)
        for i in range(A):
            part = dot(oh[i * S : (i + 1) * S], table[...])
            xs[off + i * S : off + (i + 1) * S, :] = halved(base + part)

    def forward(n):
        at = pl.ds(mo(n * TILE, TILE), TILE)
        h_buf[...] = dot(w[pl.ds(h0, HH), :], xs[at, :], NT)

        def sub(i, q):
            r = pl.ds(mo(i * SUB, SUB), SUB)
            h = h_buf[r, :]
            th = jnp.tanh(h)
            a = h * th
            vc = vcol[pl.ds(mo(h0 + i * SUB, SUB), SUB), :]
            v2 = jnp.concatenate([vc, vc], axis=1)
            so = h + a
            silu[r, at] = so.astype(bf16)
            sl[r, at] = (0.5 * v2 * ((1.0 + th) + (h - a * th))).astype(bf16)
            sv = so * v2
            return q + ((sv[0:8] + sv[8:16]) + (sv[16:24] + sv[24:32]))

        q = lax.fori_loop(0, HH // SUB, sub, jnp.zeros((8, TILE), f32), unroll=4)
        q = jnp.sum(q, axis=0, keepdims=True)
        q_sc[pl.ds(2 * n, 1), :] = q[:, 0:128]
        q_sc[pl.ds(2 * n + 1, 1), :] = q[:, 128:256]

    build(sact[...].astype(f32), obs, 0)
    each(0, 2, forward)

    each(1, PLANE, lambda k: rs_copy(k).wait_recv())
    each(1, PLANE, lambda k: qs_copy(k).wait_recv())
    r_me, c_me = tile_at(me)
    rs_buf[0] = units[r_me, c_me]
    q_buf[0] = tx_q[...]
    xr[0] = jnp.sum(rs_buf[...], axis=0)
    xq[0] = jnp.min(q_buf[...], axis=0)
    x_copies = []
    for d in (1, 2, 3):
        x_copies.append(far(xr.at[0], xr.at[d], x_s.at[d], x_r.at[d], line(d)))
        x_copies.append(far(xq.at[0], xq.at[d], xq_s.at[d], xq_r.at[d], line(d)))
    for c in x_copies:
        c.start()

    cp_obs.wait_recv()
    cp_small.wait_recv()
    obs_p = rx_obs[...].astype(f32)
    build(rx_small[0:A, 0:S], obs_p, ROWS)
    diag = jnp.where(eye, jnp.broadcast_to(rx_small[A : A + 1, 0:S], (S, S)), 0.0).astype(bf16)
    oh_p = jnp.where(dot(diag, ones) == lanes, 1.0, 0.0).astype(bf16)
    xd[S : 2 * S, :] = halved(obs_p + dot(oh_p, table[...]))
    each(2, 3, forward)

    for c in x_copies:
        c.wait_recv()
    ag_tx[0] = xr[0] + xr[2]
    ag_tx[1] = xr[1] + xr[3]

    def ag_copy(k):
        return far(ag_tx, spread.at[:, r_me, c_me], ag_s.at[k], ag_r.at[k], plane(k)[1])

    each(1, PLANE, lambda k: ag_copy(k).start())
    spread[:, r_me, c_me] = ag_tx[...]

    each(3, 4, forward)
    hd[...] = dot(w[pl.ds(h0, HH), :], xd[...], NT)
    cp_qs = far(q_sc, rx_qs, pair_s.at[4], pair_r.at[4], partner)
    cp_qs.start()
    out_l = pltpu.make_async_copy(sl, lhs_s, out_sem.at[0])
    out_l.start()

    cp_g.wait_recv()
    g_p = rx_g[...]
    norm_p = norm_of(g_p)
    units[S : 2 * S, :] = g_p / norm_p
    rt[0:COUNT, :] = (xd[...].astype(f32) * 2.0).astype(bf16)

    cp_qs.wait_recv()
    q_all = jnp.concatenate([q_sc[0:4] + rx_qs[4:8], q_sc[4:8] + rx_qs[0:4]], axis=0)
    e = jnp.exp(q_all)

    def mass(rows):
        m = row8(jnp.sum(rows, axis=0, keepdims=True))
        m = m + pltpu.roll(m, 32, 1)
        return jnp.log(m + pltpu.roll(m, 64, 1))

    mass_own, mass_p = mass(e[0:4]), mass(e[4:8])
    sub_row = iota((8, 128), 0)
    lane = iota((8, 128), 1)
    dq = jnp.exp(q_all - jnp.where(sub_row < 4, mass_own, mass_p)) * (penalty_weight / COUNT)
    for r in range(8):
        col = jnp.transpose(jnp.broadcast_to(dq[r : r + 1, :], (128, 128))) * 2.0
        for c in range(8):
            part = xs[r * 128 : (r + 1) * 128, c * 128 : (c + 1) * 128].astype(f32) * col
            x_out[r * 128 : (r + 1) * 128, c * 128 : (c + 1) * 128] = part.astype(bf16)
    out_r = pltpu.make_async_copy(x_out, rhs_s, out_sem.at[1])
    out_r.start()

    def penalty_part(i):
        r = pl.ds(mo(i * SUB, SUB), SUB)
        acc = jnp.zeros((SUB, 128), f32)
        for k in range(8):
            acc = acc + silu[r, k * 128 : (k + 1) * 128].astype(f32) * dq[k : k + 1, :]
        gw_part[r, :] = acc

    each(0, HH // SUB, penalty_part)

    cp_q.wait_recv()
    left = lane < S

    def both(own, other):
        return jnp.where(left, own, other)

    floor = both(pltpu.roll(row8(jnp.minimum(xq[0], xq[2])), 96, 1), row8(jnp.minimum(xq[1], xq[3])))
    q_data = both(row8(tx_q[...]), pltpu.roll(row8(rx_q[...]), 32, 1))
    rew = both(row8(tx_small[A + 1 : A + 2, :]), pltpu.roll(row8(rx_small[A + 1 : A + 2, :]), 32, 1))
    logp = both(row8(tx_small[A + 2 : A + 3, :]), pltpu.roll(row8(rx_small[A + 2 : A + 3, :]), 32, 1))
    target = rew + discount * (floor - entropy_temp * logp)
    td_gap = q_data - target
    dq_data = ((2.0 * td_gap - penalty_weight) * (1.0 / COUNT))[0:1, 0:COUNT]
    gap_terms = td_gap * td_gap
    mass_terms = both(mass_own, mass_p) - q_data

    each(1, PLANE, lambda k: ag_copy(k).wait_recv())
    unit = units[...]
    rest = spread[...].reshape(COUNT, D) - unit
    div_row = jnp.sum(unit * rest, axis=-1, keepdims=True)
    scale = 2.0 * diversity_weight / (COUNT - 1) / COUNT
    norms = jnp.concatenate([norm_own, norm_p], axis=0)
    dgrad = ((scale * rest - unit * (scale * div_row)) / norms).astype(bf16)
    rt[COUNT : 2 * COUNT, :] = dgrad

    def total(row):
        return jnp.sum(jnp.where(lane < COUNT, row, 0.0)[0:1], axis=1, keepdims=True)

    div_sum = jnp.sum(div_row, axis=0, keepdims=True)
    stats = jnp.where(
        lane[0:1] == 0, total(gap_terms), jnp.where(lane[0:1] == 1, total(mass_terms), div_sum)
    )
    stats_sc[...] = stats * (1.0 / COUNT)

    def tail(i):
        r = pl.ds(mo(i * 256, 256), 256)
        dc = dot(w[pl.ds(mo(h0 + i * 256, 256), 256), :], dgrad, NT)
        h = hd[r, :]
        th = jnp.tanh(h)
        a = h * th
        vc = vcol[pl.ds(mo(h0 + i * 256, 256), 256), 0:COUNT]
        slope = 0.5 * ((1.0 + th) + (h - a * th))
        curve = 0.5 * (1.0 - th * th) * (1.0 - a)
        dpre = (vc * (dq_data * slope + dc * curve)).astype(bf16)
        lt[r, :] = jnp.concatenate([dpre, (vc * slope).astype(bf16)], axis=1)
        gw_part[r, 0:COUNT] += dq_data * (h + a) + dc * slope
        for k in range(2):
            rows = pl.ds(mo(i * 256 + k * 128, 128), 128)
            gw2[b, pl.ds(2 * i + k, 1), :] = jnp.sum(jnp.transpose(gw_part[rows, :]), axis=0, keepdims=True)

    each(0, HH // 256, tail)
    cp_gw = far(gw2.at[b], gw2.at[b], pair_s.at[5], pair_r.at[5], partner)
    cp_gw.start()
    outs = [
        pltpu.make_async_copy(lt, lhs_t, out_sem.at[2]),
        pltpu.make_async_copy(rt, rhs_t, out_sem.at[3]),
        pltpu.make_async_copy(stats_sc, stats_out, out_sem.at[4]),
    ]
    for c in outs:
        c.start()
    each(1, PLANE, lambda k: rs_copy(k).wait_send())
    each(1, PLANE, lambda k: qs_copy(k).wait_send())
    each(1, PLANE, lambda k: ag_copy(k).wait_send())
    for c in x_copies + [cp_obs, cp_small, cp_g, cp_q, cp_qs]:
        c.wait_send()
    cp_gw.wait()
    out_g = pltpu.make_async_copy(gw2, gw2_out, out_sem.at[5])
    out_g.start()
    for c in outs + [out_l, out_r, out_g]:
        c.wait()


def run_main(*args):
    sds = jax.ShapeDtypeStruct
    outs = [
        sds((HH, 2 * ROWS), bf16), sds((HH, 2 * COUNT), bf16), sds((2 * ROWS, D), bf16), sds((2 * COUNT, D), bf16),
        sds((2, HH // 128, 128), f32), sds((1, 128), f32),
    ]
    vm, dma = pltpu.VMEM, pltpu.SemaphoreType.DMA
    scratch = [
        vm((NACT, D), bf16), vm((NACT, D), bf16), vm((NACT, D), bf16), vm((H, D), bf16), vm((1, H), f32),
        vm((3, 1, S), jnp.int32), vm((A, S), jnp.int32), vm((2, 1, S), f32),
        vm((2 * S, D), bf16), vm((2 * ROWS, D), bf16), vm((2 * S, D), bf16),
        vm((S, D), bf16), vm((S, D), bf16), vm((24, 128), f32), vm((24, 128), f32),
        vm((H, 128), f32), vm((S, D), f32), vm((S, D), f32), vm((1, 128), f32), vm((1, 128), f32),
        vm((COUNT, D), f32), vm((PLANE, 8, 128), f32), vm((PLANE, 1, 128), f32),
        vm((4, 8, 128), f32), vm((4, 1, 128), f32), vm((2, 8, 128), f32), vm((2, S, D), f32),
        vm((HH, TILE), f32), vm((HH, 2 * ROWS), bf16), vm((HH, 2 * ROWS), bf16), vm((HH, COUNT), f32),
        vm((8, 128), f32), vm((8, 128), f32), vm((2 * ROWS, D), bf16),
        vm((HH, 2 * COUNT), bf16), vm((2 * COUNT, D), bf16), vm((HH, 128), f32),
        vm((2, HH // 128, 128), f32), vm((1, 128), f32),
        dma((10,)), dma((NCH,)), dma((6,)), dma((6,)), dma((6,)),
        dma((PLANE,)), dma((PLANE,)), dma((PLANE,)), dma((PLANE,)),
        dma((4,)), dma((4,)), dma((4,)), dma((4,)), dma((PLANE,)), dma((PLANE,)),
    ]
    any_spec = pl.BlockSpec(memory_space=pl.ANY)
    return pl.pallas_call(
        main_kernel,
        out_shape=outs,
        in_specs=[any_spec] * len(args),
        out_specs=[any_spec] * len(outs),
        scratch_shapes=scratch,
        compiler_params=pltpu.CompilerParams(collective_id=0, has_side_effects=True, vmem_limit_bytes=60 << 20),
        name="critics",
    )(*args)


STEP = 512


def weight_kernel(lhs_s, lhs_t, rhs_s, rhs_t, gw2_in, stats_in, out, gw2, stats):
    out[0] = dot(lhs_s[...], rhs_s[...]) + dot(lhs_t[...], rhs_t[...])

    @pl.when(pl.program_id(0) == 0)
    def _():
        for k in range(2):
            for i in range(HH // 128):
                at = k * HH + i * 128
                gw2[:, at : at + 128] = gw2_in[k, i : i + 1, :]
        stats[...] = stats_in[:, 0:3]


def run_weight(*args):
    sds = jax.ShapeDtypeStruct
    once = pl.Buffered(1)
    whole = lambda *shape: pl.BlockSpec(shape, lambda i: (0,) * len(shape), pipeline_mode=once)
    return pl.pallas_call(
        weight_kernel,
        grid=(HH // STEP,),
        out_shape=[sds((1, HH, D), f32), sds((1, H), f32), sds((1, 3), f32)],
        in_specs=[
            pl.BlockSpec((STEP, 2 * ROWS), lambda i: (i, 0)),
            pl.BlockSpec((STEP, 2 * COUNT), lambda i: (i, 0)),
            whole(2 * ROWS, D), whole(2 * COUNT, D), whole(2, HH // 128, 128), whole(1, 128),
        ],
        out_specs=[
            pl.BlockSpec((1, STEP, D), lambda i: (0, i, 0)),
            pl.BlockSpec((1, H), lambda i: (0, 0)),
            pl.BlockSpec((1, 3), lambda i: (0, 0)),
        ],
        name="weights",
    )(*args)


def body(
    replay_obs, replay_next, batch_rows, data_action, next_action, sampled_actions,
    reward, next_logp, action_table, w1, w2,
):
    row = lambda x: x.reshape(1, S)
    parts = run_main(
        replay_obs, replay_next, row(batch_rows), row(data_action), row(next_action), sampled_actions.T,
        row(reward), row(next_logp), action_table, w1.reshape(H, D), w2,
    )
    return run_weight(*parts)


def solution(mesh):
    finer = Mesh(mesh.devices.reshape(4, 4, 2, 2, mesh.shape["batch"]), (*ENS, "batch"))
    placed = (
        P("batch", None), P("batch", None), P("batch"), P("batch"), P("batch"), P("batch", None),
        P("batch"), P("batch"), P(), P(ENS, None, None), P(ENS, None),
    )
    return jax.shard_map(
        body,
        mesh=finer,
        in_specs=placed,
        out_specs=(P(ENS, "batch", None), P(ENS, None), P(ENS, None)),
        check_vma=False,
    )
```

```python
import jax
import jax.numpy as jnp
from jax import lax
from jax.experimental import pallas as pl
from jax.experimental.pallas import tpu as pltpu
from jax.sharding import Mesh
from jax.sharding import PartitionSpec as P

ENS = ("ens_0", "ens_1", "ens_2", "ens_3")
MESH_ID = pl.DeviceIdType.MESH
f32, bf16 = jnp.float32, jnp.bfloat16

D, H, HH = 1024, 4096, 2048
S, A, NACT = 32, 16, 256
ROWS = S * A
CH = 1024
NCH = H // CH
BLK = 512
SUB = 32
PLANE = 32
COUNT = 64
discount, entropy_temp, penalty_weight, diversity_weight = 0.99, 0.2, 1.0, 1000.0

NN = (((1,), (0,)), ((), ()))
NT = (((1,), (1,)), ((), ()))
TN = (((0,), (0,)), ((), ()))


def dot(a, b, dims=NN):
    return lax.dot_general(a, b, dims, preferred_element_type=f32)


def mo(x, m):
    return pl.multiple_of(x, m)


def each(lo, hi, fn):
    def step(k, carry):
        fn(k)
        return carry

    lax.fori_loop(lo, hi, step, 0)


def iota(shape, dim):
    return lax.broadcasted_iota(jnp.int32, shape, dim)


def row8(x):
    return jnp.broadcast_to(x, (8, 128))


def main_kernel(
    obs_hbm, next_hbm, rows_hbm, dact_hbm, nact_hbm, sact_hbm, rew_hbm, logp_hbm, table_hbm, w_hbm, v_hbm,
    part, lt, rt, gw2, stats_out,
    tab_obs, tab_next, table, w, v, ids, sact, rl,
    xdn, xs, xd, tx_obs, rx_obs, tx_small, rx_small,
    vcol, ho, gin, rx_g, tx_q, rx_q, units, rs_tx, rs_buf, xr, ag_tx, spread,
    h_buf, sl, silu, q_sc, rx_qs, x_out, tail_x, tail_r,
    in_sem, w_sem, pair_s, pair_r, rs_s, rs_r, x_s, x_r, ag_s, ag_r,
):
    z, y, xh, core = (lax.axis_index(n) for n in ENS)
    b = lax.axis_index("batch")
    me = z * 8 + y * 2 + core
    xpos = xh * 2 + b

    def plane(k):
        j = lax.rem(me + k, PLANE)
        return j, (lax.div(j, 8), lax.rem(lax.div(j, 2), 4), xh, lax.rem(j, 2), b)

    def line(d):
        p = lax.rem(xpos + d, 4)
        return (z, y, lax.div(p, 2), core, lax.rem(p, 2))

    partner = (z, y, xh, core, 1 - b)
    h0 = mo(b * HH, HH)

    def far(src, dst, ssem, rsem, device):
        return pltpu.make_async_remote_copy(
            src_ref=src, dst_ref=dst, send_sem=ssem, recv_sem=rsem, device_id=device, device_id_type=MESH_ID
        )

    loads = [
        pltpu.make_async_copy(src, dst, in_sem.at[i])
        for i, (src, dst) in enumerate(
            [
                (rows_hbm, ids.at[0]), (dact_hbm, ids.at[1]), (nact_hbm, ids.at[2]), (sact_hbm, sact),
                (rew_hbm, rl.at[0]), (logp_hbm, rl.at[1]),
                (obs_hbm, tab_obs), (table_hbm, table), (next_hbm, tab_next), (v_hbm, v),
            ]
        )
    ]
    for c in loads:
        c.start()

    def w_copy(c):
        at = pl.ds(c * CH, CH)
        return pltpu.make_async_copy(w_hbm.at[at], w.at[at], w_sem.at[c])

    for c in range(NCH):
        w_copy(c).start()

    barrier = pltpu.get_barrier_semaphore()

    def greet(device):
        pl.semaphore_signal(barrier, inc=1, device_id=device, device_id_type=MESH_ID)

    each(1, PLANE, lambda k: greet(plane(k)[1]))
    for d in (1, 2, 3):
        greet(line(d))

    for c in loads[:6]:
        c.wait()

    lanes = iota((S, NACT), 1).astype(f32)
    eye = iota((S, S), 0) == iota((S, S), 1)
    ones = jnp.ones((S, NACT), bf16)

    def one_hot(row, value):
        diag = jnp.where(eye, jnp.broadcast_to(row, (S, S)), 0.0).astype(bf16)
        return jnp.where(dot(diag, ones) == lanes, value, 0.0).astype(bf16)

    def sample_hot(sact_f):
        pick = jnp.where((iota((ROWS, S), 0) & (S - 1)) == iota((ROWS, S), 1), 1.0, 0.0).astype(bf16)
        each_sample = dot(pick, sact_f.astype(bf16), NT)
        mine = lax.shift_right_logical(iota((ROWS, A), 0), 5) == iota((ROWS, A), 1)
        index = dot(jnp.where(mine, each_sample, 0.0).astype(bf16), jnp.ones((A, NACT), bf16))
        return jnp.where(index == iota((ROWS, NACT), 1).astype(f32), 0.5, 0.0).astype(bf16)

    rows_oh, dact_oh, nact_oh = (one_hot(ids[i].astype(f32), 0.5) for i in range(3))
    own_hot = sample_hot(sact[...].astype(f32))
    tx_small[...] = jnp.zeros_like(tx_small)
    tx_small[0:A, 0:S] = sact[...].astype(f32)
    tx_small[A : A + 1, 0:S] = ids[1].astype(f32)
    tx_small[A + 1 : A + 2, 0:S] = rl[0]
    tx_small[A + 2 : A + 3, 0:S] = rl[1]
    for c in loads[6:]:
        c.wait()

    obs = dot(rows_oh, tab_obs[...])
    nxt = dot(rows_oh, tab_next[...])
    tx_obs[...] = obs.astype(bf16)
    half_data = (obs + dot(dact_oh, table[...])).astype(bf16)
    xdn[0:S, :] = half_data
    xdn[S : 2 * S, :] = (nxt + dot(nact_oh, table[...])).astype(bf16)
    xd[0:S, :] = half_data

    def own_act(c, q_acc):
        at = slice(c * CH, (c + 1) * CH)
        h = ho[:, at]
        th = jnp.tanh(h)
        a = h * th
        vr = v[:, at]
        sv = (h + a) * vr
        for k in range(CH // 128):
            q_acc = q_acc + sv[:, k * 128 : (k + 1) * 128]
        hs, ts = h[0:S], th[0:S]
        co = (0.5 * vr * ((1.0 + ts) + (hs - a[0:S] * ts))).astype(bf16)
        g = dot(co, w[at, :])
        gin[...] = g if c == 0 else gin[...] + g
        return q_acc

    def spread_v(i):
        at = pl.ds(mo(h0 + i * 128, 128), 128)
        vcol[i * 128 : (i + 1) * 128, :] = jnp.transpose(jnp.broadcast_to(v[:, at], (128, 128)))

    q_acc = jnp.zeros((2 * S, 128), f32)
    cp_obs = far(tx_obs, rx_obs, pair_s.at[0], pair_r.at[0], partner)
    cp_small = far(tx_small, rx_small, pair_s.at[1], pair_r.at[1], partner)
    for c in range(NCH):
        w_copy(c).wait()
        ho[:, c * CH : (c + 1) * CH] = dot(xdn[...], w[c * CH : (c + 1) * CH, :], NT)
        if c > 0:
            q_acc = own_act(c - 1, q_acc)
        for i in range(4):
            spread_v(4 * c + i)
        if c == 2:
            pl.semaphore_wait(barrier, PLANE - 1 + 3)
            cp_obs.start()
            cp_small.start()
    q_acc = own_act(NCH - 1, q_acc)
    q_own = jnp.sum(jnp.transpose(jnp.concatenate([q_acc, jnp.zeros((64, 128), f32)], axis=0)), axis=0, keepdims=True)
    tx_q[...] = q_own

    def norm_of(g):
        return jnp.sqrt(jnp.sum(g * g, axis=-1, keepdims=True) + 1.0)

    g_own = gin[...]
    norm_own = norm_of(g_own)
    u_own = g_own / norm_own
    units[0:S, :] = u_own
    for j in range(PLANE):
        r, c = j // 8, j % 8
        rs_tx[j, 0:8, :] = u_own[8 * r : 8 * r + 8, 128 * c : 128 * c + 128]
        rs_tx[j, 8:9, :] = q_own

    def rs_copy(k):
        j, device = plane(k)
        return far(rs_tx.at[j], rs_buf.at[k], rs_s.at[k], rs_r.at[k], device)

    each(1, PLANE, lambda k: rs_copy(k).start())
    cp_g = far(gin, rx_g, pair_s.at[2], pair_r.at[2], partner)
    cp_q = far(tx_q, rx_q, pair_s.at[3], pair_r.at[3], partner)
    cp_g.start()
    cp_q.start()

    def build(hot, base, off):
        for p in range(2):
            h_buf[p] = dot(hot, table[:, p * 512 : (p + 1) * 512])
        for i in range(A):
            for p in range(2):
                x = (base[:, p * 512 : (p + 1) * 512] + h_buf[p, i * S : (i + 1) * S, :]).astype(bf16)
                xs[off + i * S : off + (i + 1) * S, p * 512 : (p + 1) * 512] = x

    def product(m, half):
        h_buf[m % 2] = dot(w[pl.ds(mo(h0 + m * BLK, BLK), BLK), :], xs[half * ROWS : (half + 1) * ROWS, :], NT)

    def activate(m, half, q):
        at = slice(half * ROWS, (half + 1) * ROWS)
        for i in range(BLK // SUB):
            h = h_buf[m % 2, i * SUB : (i + 1) * SUB, :]
            r = slice(m * BLK + i * SUB, m * BLK + (i + 1) * SUB)
            th = jnp.tanh(h)
            a = h * th
            vc = vcol[r, :]
            v4 = jnp.concatenate([vc, vc, vc, vc], axis=1)
            so = h + a
            silu[r, at] = so.astype(bf16)
            sl[r, at] = (0.5 * v4 * ((1.0 + th) + (h - a * th))).astype(bf16)
            sv = so * v4
            q = q + ((sv[0:8] + sv[8:16]) + (sv[16:24] + sv[24:32]))
        return q

    def keep_q(q, half):
        q = jnp.sum(q, axis=0, keepdims=True)
        for k in range(4):
            q_sc[4 * half + k : 4 * half + k + 1, :] = q[:, k * 128 : (k + 1) * 128]

    nb = HH // BLK
    q_zero = jnp.zeros((8, ROWS), f32)

    def forward(half):
        product(0, half)
        q = q_zero
        for m in range(1, nb):
            product(m, half)
            q = activate(m - 1, half, q)
        keep_q(activate(nb - 1, half, q), half)

    build(own_hot, obs, 0)
    forward(0)

    cp_obs.wait_recv()
    cp_small.wait_recv()
    obs_p = rx_obs[...].astype(f32)
    build(sample_hot(rx_small[0:A, 0:S]), obs_p, ROWS)
    half_p = (obs_p + dot(one_hot(rx_small[A : A + 1, 0:S], 0.5), table[...])).astype(bf16)
    xd[S : 2 * S, :] = half_p
    tail_x[COUNT : COUNT + S, :] = half_p
    forward(1)
    cp_qs = far(q_sc, rx_qs, pair_s.at[4], pair_r.at[4], partner)
    cp_qs.start()

    each(1, PLANE, lambda k: rs_copy(k).wait_recv())
    rs_buf[0] = rs_tx[me]
    got = rs_buf[...]
    xr[0, 0:8, :] = jnp.sum(got[:, 0:8, :], axis=0)
    xr[0, 8:9, :] = jnp.min(got[:, 8:9, :], axis=0)
    x_copies = [far(xr.at[0], xr.at[d], x_s.at[d], x_r.at[d], line(d)) for d in (1, 2, 3)]
    for c in x_copies:
        c.start()

    cp_g.wait_recv()
    g_p = rx_g[...]
    norm_p = norm_of(g_p)
    units[S : 2 * S, :] = g_p / norm_p
    rt[0:COUNT, :] = (xd[...].astype(f32) * 2.0).astype(bf16)

    cp_qs.wait_recv()
    q_all = jnp.concatenate([q_sc[0:4] + rx_qs[4:8], q_sc[4:8] + rx_qs[0:4]], axis=0)
    e = jnp.exp(q_all)

    def mass(rows):
        m = row8(jnp.sum(rows, axis=0, keepdims=True))
        m = m + pltpu.roll(m, 32, 1)
        return jnp.log(m + pltpu.roll(m, 64, 1))

    mass_own, mass_p = mass(e[0:4]), mass(e[4:8])
    sub_row = iota((8, 128), 0)
    lane = iota((8, 128), 1)
    dq = jnp.exp(q_all - jnp.where(sub_row < 4, mass_own, mass_p)) * (penalty_weight / COUNT)
    for r in range(8):
        col = jnp.transpose(jnp.broadcast_to(dq[r : r + 1, :], (128, 128))) * 2.0
        for c in range(8):
            scaled = xs[r * 128 : (r + 1) * 128, c * 128 : (c + 1) * 128].astype(f32) * col
            x_out[r * 128 : (r + 1) * 128, c * 128 : (c + 1) * 128] = scaled.astype(bf16)

    for c in x_copies:
        c.wait_recv()
    row_me = mo(lax.div(me, 8) * 16, 16)
    col_me = mo(lax.rem(me, 8) * 128, 128)
    ag_tx[...] = jnp.concatenate([xr[0, 0:8, :] + xr[2, 0:8, :], xr[1, 0:8, :] + xr[3, 0:8, :]], axis=0).astype(bf16)

    def ag_copy(k):
        dst = spread.at[pl.ds(row_me, 16), pl.ds(col_me, 128)]
        return far(ag_tx, dst, ag_s.at[k], ag_r.at[k], plane(k)[1])

    each(1, PLANE, lambda k: ag_copy(k).start())
    spread[pl.ds(row_me, 16), pl.ds(col_me, 128)] = ag_tx[...]

    dq_row = jnp.concatenate([dq[r : r + 1, :] for r in range(8)], axis=1)
    dq_hi = dq_row.astype(bf16).astype(f32)
    dq_two = jnp.concatenate([dq_hi, dq_row - dq_hi, jnp.zeros((14, 2 * ROWS), f32)], axis=0).astype(bf16)
    gw_s = dot(dq_two, silu[...], NT)
    gw_s = gw_s[0:1] + gw_s[1:2]
    for m in range(nb):
        r = slice(m * BLK, (m + 1) * BLK)
        part[r, :] = dot(sl[r, :], x_out[...])

    cp_q.wait_recv()
    left = lane < S

    def both(own, other):
        return jnp.where(left, own, other)

    floor_own, floor_p = jnp.minimum(xr[0, 8:9, :], xr[2, 8:9, :]), jnp.minimum(xr[1, 8:9, :], xr[3, 8:9, :])
    floor = both(pltpu.roll(row8(floor_own), 96, 1), row8(floor_p))
    q_data = both(row8(tx_q[...]), pltpu.roll(row8(rx_q[...]), 32, 1))
    rew = both(row8(tx_small[A + 1 : A + 2, :]), pltpu.roll(row8(rx_small[A + 1 : A + 2, :]), 32, 1))
    logp = both(row8(tx_small[A + 2 : A + 3, :]), pltpu.roll(row8(rx_small[A + 2 : A + 3, :]), 32, 1))
    target = rew + discount * (floor - entropy_temp * logp)
    td_gap = q_data - target
    gap_terms = td_gap * td_gap
    mass_terms = both(mass_own, mass_p) - q_data
    dq_data = ((2.0 * td_gap - penalty_weight) * (1.0 / COUNT))[0:1]
    dq_col = jnp.transpose(jnp.broadcast_to(dq_data, (128, 128)))[0:COUNT]
    dq_col = jnp.concatenate([dq_col] * (BLK // 128), axis=1)

    each(1, PLANE, lambda k: ag_copy(k).wait_recv())
    unit = units[...]
    got_sum = spread[...].astype(f32)
    own_rows = [got_sum[16 * r : 16 * r + 8] for r in range(4)]
    other_rows = [got_sum[16 * r + 8 : 16 * r + 16] for r in range(4)]
    rest = jnp.concatenate(own_rows + other_rows, axis=0) - unit
    div_row = jnp.sum(unit * rest, axis=-1, keepdims=True)
    scale = 2.0 * diversity_weight / (COUNT - 1) / COUNT
    norms = jnp.concatenate([norm_own, norm_p], axis=0)
    dgrad = ((scale * rest - unit * (scale * div_row)) / norms).astype(bf16)
    rt[COUNT : 2 * COUNT, :] = dgrad
    tail_x[0:COUNT, :] = dgrad

    def total(row):
        return jnp.sum(jnp.where(lane < COUNT, row, 0.0)[0:1], axis=1, keepdims=True)

    div_sum = jnp.sum(div_row, axis=0, keepdims=True)
    first = lane[0:1]
    stats = jnp.where(first == 0, total(gap_terms), jnp.where(first == 1, total(mass_terms), div_sum))
    stats_out[...] = stats * (1.0 / COUNT)

    def pieces(m):
        at = slice(m * BLK, (m + 1) * BLK)
        far_at = pl.ds(mo(h0 + m * BLK, BLK), BLK)
        h = jnp.concatenate([ho[0:S, far_at], tail_r[COUNT : COUNT + S, at]], axis=0)
        th = jnp.tanh(h)
        a = h * th
        return at, far_at, h, th, a, 0.5 * ((1.0 + th) + (h - a * th)), tail_r[0:COUNT, at]

    for m in range(nb):
        tail_r[:, m * BLK : (m + 1) * BLK] = dot(tail_x[...], w[pl.ds(mo(h0 + m * BLK, BLK), BLK), :], NT)
    for m in range(nb):
        at, far_at, h, th, a, slope, dc = pieces(m)
        gw2[:, far_at] = gw_s[:, at] + jnp.sum(dq_col * (h + a) + dc * slope, axis=0, keepdims=True)
    gw_at = pl.ds(h0, HH)
    cp_gw = far(gw2.at[:, gw_at], gw2.at[:, gw_at], pair_s.at[5], pair_r.at[5], partner)
    cp_gw.start()
    for m in range(nb):
        at, far_at, h, th, a, slope, dc = pieces(m)
        vr = v[:, far_at]
        curve = 0.5 * (1.0 - th * th) * (1.0 - a)
        lt[0:COUNT, at] = (vr * (dq_col * slope + dc * curve)).astype(bf16)
        lt[COUNT : 2 * COUNT, at] = (vr * slope).astype(bf16)
    each(1, PLANE, lambda k: rs_copy(k).wait_send())
    each(1, PLANE, lambda k: ag_copy(k).wait_send())
    for c in x_copies + [cp_obs, cp_small, cp_g, cp_q, cp_qs]:
        c.wait_send()
    cp_gw.wait()
    return None


def run_main(*args):
    vm, dma = pltpu.VMEM, pltpu.SemaphoreType.DMA
    outs = [
        vm((HH, D), f32), vm((2 * COUNT, HH), bf16), vm((2 * COUNT, D), bf16), vm((1, H), f32), vm((1, 128), f32),
    ]
    scratch = [
        vm((NACT, D), bf16), vm((NACT, D), bf16), vm((NACT, D), bf16), vm((H, D), bf16), vm((1, H), f32),
        vm((3, 1, S), jnp.int32), vm((A, S), jnp.int32), vm((2, 1, S), f32),
        vm((2 * S, D), bf16), vm((2 * ROWS, D), bf16), vm((2 * S, D), bf16),
        vm((S, D), bf16), vm((S, D), bf16), vm((24, 128), f32), vm((24, 128), f32),
        vm((HH, 128), f32), vm((2 * S, H), f32), vm((S, D), f32), vm((S, D), f32), vm((1, 128), f32), vm((1, 128), f32),
        vm((COUNT, D), f32), vm((PLANE, 9, 128), f32), vm((PLANE, 9, 128), f32),
        vm((4, 9, 128), f32), vm((16, 128), bf16), vm((COUNT, D), bf16),
        vm((2, BLK, ROWS), f32), vm((HH, 2 * ROWS), bf16), vm((HH, 2 * ROWS), bf16),
        vm((8, 128), f32), vm((8, 128), f32), vm((2 * ROWS, D), bf16), vm((COUNT + S, D), bf16), vm((COUNT + S, HH), f32),
        dma((10,)), dma((NCH,)), dma((6,)), dma((6,)),
        dma((PLANE,)), dma((PLANE,)), dma((4,)), dma((4,)), dma((PLANE,)), dma((PLANE,)),
    ]
    return pl.pallas_call(
        main_kernel,
        out_shape=outs,
        in_specs=[pl.BlockSpec(memory_space=pltpu.HBM)] * len(args),
        out_specs=[pl.BlockSpec(memory_space=pltpu.VMEM)] * len(outs),
        scratch_shapes=scratch,
        compiler_params=pltpu.CompilerParams(collective_id=0, has_side_effects=True, vmem_limit_bytes=40 << 20),
        name="critics",
    )(*(pltpu.with_memory_space_constraint(a, pltpu.HBM) for a in args))


STEP = 256


def weight_kernel(part, lt, rt, gw2_in, stats_in, out, gw2, stats, buf, stats_sc, sems):
    stats_sc[...] = stats_in[:, 0:3]
    copies = [pltpu.make_async_copy(gw2_in, gw2, sems.at[0]), pltpu.make_async_copy(stats_sc, stats, sems.at[1])]
    for c in copies:
        c.start()
    for i in range(HH // STEP):
        r = slice(i * STEP, (i + 1) * STEP)
        buf[r, :] = part[r, :] + dot(lt[:, r], rt[...], TN)
        c = pltpu.make_async_copy(buf.at[pl.ds(i * STEP, STEP)], out.at[0, pl.ds(i * STEP, STEP)], sems.at[2 + i])
        c.start()
        copies.append(c)
    for c in copies:
        c.wait()


def run_weight(*args):
    sds = jax.ShapeDtypeStruct
    hbm = pl.BlockSpec(memory_space=pltpu.HBM)
    return pl.pallas_call(
        weight_kernel,
        out_shape=[sds((1, HH, D), f32), sds((1, H), f32), sds((1, 3), f32)],
        in_specs=[pl.BlockSpec(memory_space=pltpu.VMEM)] * len(args),
        out_specs=[hbm] * 3,
        scratch_shapes=[
            pltpu.VMEM((HH, D), f32), pltpu.VMEM((1, 3), f32), pltpu.SemaphoreType.DMA((2 + HH // STEP,)),
        ],
        compiler_params=pltpu.CompilerParams(vmem_limit_bytes=20 << 20),
        name="weights",
    )(*args)


def body(
    replay_obs, replay_next, batch_rows, data_action, next_action, sampled_actions,
    reward, next_logp, action_table, w1, w2,
):
    row = lambda x: x.reshape(1, S)
    parts = run_main(
        replay_obs, replay_next, row(batch_rows), row(data_action), row(next_action), sampled_actions.T,
        row(reward), row(next_logp), action_table, w1.reshape(H, D), w2,
    )
    return run_weight(*parts)


def solution(mesh):
    finer = Mesh(mesh.devices.reshape(4, 4, 2, 2, mesh.shape["batch"]), (*ENS, "batch"))
    placed = (
        P("batch", None), P("batch", None), P("batch"), P("batch"), P("batch"), P("batch", None),
        P("batch"), P("batch"), P(), P(ENS, None, None), P(ENS, None),
    )
    return jax.shard_map(
        body,
        mesh=finer,
        in_specs=placed,
        out_specs=(P(ENS, "batch", None), P(ENS, None), P(ENS, None)),
        check_vma=False,
    )
```

```python
import jax
import jax.numpy as jnp
from jax import lax
from jax.experimental import pallas as pl
from jax.experimental.pallas import tpu as pltpu
from jax.sharding import Mesh
from jax.sharding import PartitionSpec as P

ENS = ("ens_0", "ens_1", "ens_2", "ens_3")
MESH_ID = pl.DeviceIdType.MESH
f32, bf16 = jnp.float32, jnp.bfloat16

D, H, HH = 1024, 4096, 2048
S, A, NACT = 32, 16, 256
ROWS = S * A
CH = 512
NCH = H // CH
BLK = 512
SUB = 32
PLANE = 32
COUNT = 64
discount, entropy_temp, penalty_weight, diversity_weight = 0.99, 0.2, 1.0, 1000.0

NN = (((1,), (0,)), ((), ()))
NT = (((1,), (1,)), ((), ()))
TN = (((0,), (0,)), ((), ()))


def dot(a, b, dims=NN):
    return lax.dot_general(a, b, dims, preferred_element_type=f32)


def mo(x, m):
    return pl.multiple_of(x, m)


def each(lo, hi, fn):
    def step(k, carry):
        fn(k)
        return carry

    lax.fori_loop(lo, hi, step, 0)


def iota(shape, dim):
    return lax.broadcasted_iota(jnp.int32, shape, dim)


def row8(x):
    return jnp.broadcast_to(x, (8, 128))


def main_kernel(
    obs_hbm, next_hbm, rows_hbm, dact_hbm, nact_hbm, sact_hbm, rew_hbm, logp_hbm, table_hbm, w_hbm, v_hbm,
    part, w, rt, tail_x, ho, v, gw2, dq_out, stats_out,
    tab_obs, tab_next, table, ids, sact, rl,
    xdn, xs, xd, tx_obs, rx_obs, tx_small, rx_small,
    vcol, h_next, gin, rx_g, tx_q, rx_q, units, rs_tx, rs_buf, xr, ag_tx, spread,
    h_buf, sl, silu, q_own_sc, q_far_sc, rx_q_own, rx_q_far, x_out, gw_part,
    in_sem, w_sem, pair_s, pair_r, x_s, x_r, many,
):
    z, y, xh, core = (lax.axis_index(n) for n in ENS)
    b = lax.axis_index("batch")
    me = z * 8 + y * 2 + core
    xpos = xh * 2 + b

    zs = [lax.rem(z + d, 4) for d in range(4)]
    ys = [lax.rem(y + d, 4) for d in range(4)]
    cores = [core, 1 - core]
    order = sorted(range(1, PLANE), key=lambda k: -((0, 1, 2, 1)[k // 8] + (0, 1, 2, 1)[k // 2 % 4]))

    def plane(k):
        pz, py, pc = zs[k // 8], ys[k // 2 % 4], cores[k % 2]
        return pz * 8 + py * 2 + pc, (pz, py, xh, pc, b)

    def line(d):
        p = lax.rem(xpos + d, 4)
        return (z, y, lax.div(p, 2), core, lax.rem(p, 2))

    partner = (z, y, xh, core, 1 - b)
    h0 = mo(b * HH, HH)

    def far(src, dst, ssem, rsem, device):
        return pltpu.make_async_remote_copy(
            src_ref=src, dst_ref=dst, send_sem=ssem, recv_sem=rsem, device_id=device, device_id_type=MESH_ID
        )

    loads = [
        pltpu.make_async_copy(src, dst, in_sem.at[i])
        for i, (src, dst) in enumerate(
            [
                (rows_hbm, ids.at[0]), (dact_hbm, ids.at[1]), (nact_hbm, ids.at[2]), (sact_hbm, sact),
                (rew_hbm, rl.at[0]), (logp_hbm, rl.at[1]),
                (obs_hbm, tab_obs), (table_hbm, table), (next_hbm, tab_next), (v_hbm, v),
            ]
        )
    ]
    for c in loads:
        c.start()

    def w_copy(c):
        at = pl.ds(c * CH, CH)
        return pltpu.make_async_copy(w_hbm.at[at], w.at[at], w_sem.at[c])

    barrier = pltpu.get_barrier_semaphore()

    def greet(device):
        pl.semaphore_signal(barrier, inc=1, device_id=device, device_id_type=MESH_ID)

    for k in order:
        greet(plane(k)[1])
    for d in (1, 2, 3):
        greet(line(d))
    for c in range(4):
        w_copy(c).start()

    for c in loads[:6]:
        c.wait()

    lanes = iota((S, NACT), 1).astype(f32)
    eye = iota((S, S), 0) == iota((S, S), 1)
    ones = jnp.ones((S, NACT), bf16)

    def one_hot(row, value):
        diag = jnp.where(eye, jnp.broadcast_to(row, (S, S)), 0.0).astype(bf16)
        return jnp.where(dot(diag, ones) == lanes, value, 0.0).astype(bf16)

    def sample_hot(sact_f):
        pick = jnp.where((iota((ROWS, S), 0) & (S - 1)) == iota((ROWS, S), 1), 1.0, 0.0).astype(bf16)
        each_sample = dot(pick, sact_f.astype(bf16), NT)
        mine = lax.shift_right_logical(iota((ROWS, A), 0), 5) == iota((ROWS, A), 1)
        index = dot(jnp.where(mine, each_sample, 0.0).astype(bf16), jnp.ones((A, NACT), bf16))
        return jnp.where(index == iota((ROWS, NACT), 1).astype(f32), 0.5, 0.0).astype(bf16)

    rows_oh, dact_oh, nact_oh = (one_hot(ids[i].astype(f32), 0.5) for i in range(3))
    own_hot = sample_hot(sact[...].astype(f32))
    tx_small[...] = jnp.zeros_like(tx_small)
    tx_small[0:A, 0:S] = sact[...].astype(f32)
    tx_small[A : A + 1, 0:S] = ids[1].astype(f32)
    tx_small[A + 1 : A + 2, 0:S] = rl[0]
    tx_small[A + 2 : A + 3, 0:S] = rl[1]
    for c in loads[6:]:
        c.wait()
    for c in range(4, NCH):
        w_copy(c).start()

    obs = dot(rows_oh, tab_obs[...])
    nxt = dot(rows_oh, tab_next[...])
    tx_obs[...] = obs.astype(bf16)
    half_data = (obs + dot(dact_oh, table[...])).astype(bf16)
    xdn[0:S, :] = half_data
    xdn[S : 2 * S, :] = (nxt + dot(nact_oh, table[...])).astype(bf16)
    xd[0:S, :] = half_data

    def own_act(c, q_acc):
        at = slice(c * CH, (c + 1) * CH)
        h = jnp.concatenate([ho[:, at], h_next[c % 2]], axis=0)
        th = jnp.tanh(h)
        p = 1.0 + th
        so = h * p
        vr = v[:, at]
        sv = so * vr
        for k in range(CH // 128):
            q_acc = q_acc + sv[:, k * 128 : (k + 1) * 128]
        co = (0.5 * vr * (p[0:S] + so[0:S] * (1.0 - th[0:S]))).astype(bf16)
        g = dot(co, w[at, :])
        gin[...] = g if c == 0 else gin[...] + g
        return q_acc

    def spread_v(i):
        at = pl.ds(mo(h0 + i * 128, 128), 128)
        vcol[i * 128 : (i + 1) * 128, :] = jnp.transpose(jnp.broadcast_to(0.5 * v[:, at], (128, 128)))

    q_acc = jnp.zeros((2 * S, 128), f32)
    cp_obs = far(tx_obs, rx_obs, pair_s.at[0], pair_r.at[0], partner)
    cp_small = far(tx_small, rx_small, pair_s.at[1], pair_r.at[1], partner)
    for c in range(NCH):
        if c % 2 == 0:
            w_copy(c).wait()
            w_copy(c + 1).wait()
        h = dot(xdn[...], w[c * CH : (c + 1) * CH, :], NT)
        ho[:, c * CH : (c + 1) * CH] = h[0:S]
        h_next[c % 2] = h[S : 2 * S]
        if c > 0:
            q_acc = own_act(c - 1, q_acc)
        for i in range(2):
            spread_v(2 * c + i)
    q_acc = own_act(NCH - 1, q_acc)
    q_own = jnp.sum(jnp.transpose(jnp.concatenate([q_acc, jnp.zeros((64, 128), f32)], axis=0)), axis=0, keepdims=True)
    tx_q[...] = q_own

    def norm_of(g):
        return jnp.sqrt(jnp.sum(g * g, axis=-1, keepdims=True) + 1.0)

    g_own = gin[...]
    norm_own = norm_of(g_own)
    u_own = g_own / norm_own
    units[0:S, :] = u_own
    q_hi = q_own.astype(bf16).astype(f32)
    q_mid = (q_own - q_hi).astype(bf16).astype(f32)
    q_rows = jnp.concatenate([q_hi, q_mid, q_own - q_hi - q_mid, jnp.zeros((5, 128), f32)], axis=0)
    for j in range(PLANE):
        r, c = j // 8, j % 8
        u_tile = u_own[8 * r : 8 * r + 8, 128 * c : 128 * c + 128]
        rs_tx[j] = jnp.concatenate([u_tile, q_rows], axis=0).astype(bf16)

    def rs_copy(k):
        j, device = plane(k)
        return far(rs_tx.at[j], rs_buf.at[k], many.at[0], many.at[1], device)

    all_in = rs_buf.at[pl.ds(1, PLANE - 1)]
    rs_all = far(all_in, all_in, many.at[0], many.at[1], partner)
    pl.semaphore_wait(barrier, PLANE - 1 + 3)
    for k in order:
        rs_copy(k).start()
    cp_obs.start()
    cp_small.start()
    cp_g = far(gin, rx_g, pair_s.at[2], pair_r.at[2], partner)
    cp_q = far(tx_q, rx_q, pair_s.at[3], pair_r.at[3], partner)
    cp_g.start()
    cp_q.start()

    def build(hot, base, off):
        for p in range(2):
            h_buf[p] = dot(hot, table[:, p * 512 : (p + 1) * 512])
        for i in range(A):
            for p in range(2):
                x = (base[:, p * 512 : (p + 1) * 512] + h_buf[p, i * S : (i + 1) * S, :]).astype(bf16)
                xs[off + i * S : off + (i + 1) * S, p * 512 : (p + 1) * 512] = x

    nb = HH // BLK

    def product(n):
        half, m = divmod(n, nb)
        h_buf[m] = dot(w[pl.ds(mo(h0 + m * BLK, BLK), BLK), :], xs[half * ROWS : (half + 1) * ROWS, :], NT)

    def activate(n, q):
        half, m = divmod(n, nb)
        at = slice(half * ROWS, (half + 1) * ROWS)
        for i in range(BLK // SUB):
            h = h_buf[m, i * SUB : (i + 1) * SUB, :]
            r = slice(m * BLK + i * SUB, m * BLK + (i + 1) * SUB)
            th = jnp.tanh(h)
            p = 1.0 + th
            so = h * p
            vh = vcol[r, :]
            vh = jnp.concatenate([vh, vh, vh, vh], axis=1)
            silu[r, at] = so.astype(bf16)
            sl[r, at] = (vh * (p + so * (1.0 - th))).astype(bf16)
            sv = so * vh
            q = q + ((sv[0:8] + sv[8:16]) + (sv[16:24] + sv[24:32]))
        return q

    def keep_q(q, ref):
        q = 2.0 * jnp.sum(q, axis=0, keepdims=True)
        for k in range(4):
            ref[k : k + 1, :] = q[:, k * 128 : (k + 1) * 128]

    q_zero = jnp.zeros((8, ROWS), f32)
    cp_q_own = far(q_own_sc, rx_q_own, pair_s.at[4], pair_r.at[4], partner)
    cp_q_far = far(q_far_sc, rx_q_far, pair_s.at[5], pair_r.at[5], partner)
    x_copies = [far(xr.at[0], xr.at[d], x_s.at[d - 1], x_r.at[d - 1], line(d)) for d in (1, 2, 3)]

    build(own_hot, obs, 0)
    product(0)
    q = q_zero
    for n in range(1, nb):
        product(n)
        q = activate(n - 1, q)

    cp_obs.wait_recv()
    cp_small.wait_recv()
    obs_p = rx_obs[...].astype(f32)
    build(sample_hot(rx_small[0:A, 0:S]), obs_p, ROWS)
    half_p = (obs_p + dot(one_hot(rx_small[A : A + 1, 0:S], 0.5), table[...])).astype(bf16)
    xd[S : 2 * S, :] = half_p
    tail_x[COUNT : COUNT + S, :] = half_p
    product(nb)
    keep_q(activate(nb - 1, q), q_own_sc)

    rs_all.wait_recv()
    rs_buf[0] = rs_tx[me]
    got = rs_buf[...].astype(f32)
    xr[0, 0:8, :] = jnp.sum(got[:, 0:8, :], axis=0)
    xr[0, 8:9, :] = jnp.min((got[:, 8:9, :] + got[:, 9:10, :]) + got[:, 10:11, :], axis=0)
    for c in x_copies:
        c.start()
    cp_q_own.start()
    q = q_zero
    for n in range(nb + 1, 2 * nb):
        product(n)
        q = activate(n - 1, q)

    keep_q(activate(2 * nb - 1, q), q_far_sc)
    cp_q_far.start()

    for c in x_copies:
        c.wait_recv()
    row_me = mo(lax.div(me, 8) * 16, 16)
    col_me = mo(lax.rem(me, 8) * 128, 128)
    ag_tx[...] = jnp.concatenate([xr[0, 0:8, :] + xr[2, 0:8, :], xr[1, 0:8, :] + xr[3, 0:8, :]], axis=0).astype(bf16)

    def ag_copy(k):
        dst = spread.at[pl.ds(row_me, 16), pl.ds(col_me, 128)]
        return far(ag_tx, dst, many.at[2], many.at[3], plane(k)[1])

    ag_all = far(all_in, all_in, many.at[2], many.at[3], partner)

    for k in order:
        ag_copy(k).start()
    spread[pl.ds(row_me, 16), pl.ds(col_me, 128)] = ag_tx[...]

    cp_g.wait_recv()
    g_p = rx_g[...]
    norm_p = norm_of(g_p)
    units[S : 2 * S, :] = g_p / norm_p
    rt[0:COUNT, :] = (xd[...].astype(f32) * 2.0).astype(bf16)

    def penalty(q4, half):
        m = row8(jnp.sum(jnp.exp(q4), axis=0, keepdims=True))
        m = m + pltpu.roll(m, 32, 1)
        mass = jnp.log(m + pltpu.roll(m, 64, 1))
        dq = jnp.exp(q4 - mass[0:4]) * (penalty_weight / COUNT)
        for r in range(4):
            col = jnp.transpose(jnp.broadcast_to(dq[r : r + 1, :], (128, 128))) * 2.0
            rows = slice(half * ROWS + r * 128, half * ROWS + (r + 1) * 128)
            for c in range(8):
                at = slice(c * 128, (c + 1) * 128)
                x_out[rows, at] = (xs[rows, at].astype(f32) * col).astype(bf16)
        return mass, dq

    def weight_part(m, half, first):
        at = slice(half * ROWS, (half + 1) * ROWS)
        r = slice(m * BLK, (m + 1) * BLK)
        g = dot(sl[r, at], x_out[at, :])
        part[r, :] = g if first else part[r, :] + g

    def readout_part(m, dq, half, first):
        for i in range(BLK // SUB):
            r = slice(m * BLK + i * SUB, m * BLK + (i + 1) * SUB)
            acc = None if first else gw_part[r, :]
            for k in range(4):
                c = slice(half * ROWS + k * 128, half * ROWS + (k + 1) * 128)
                term = silu[r, c].astype(f32) * dq[k : k + 1, :]
                acc = term if acc is None else acc + term
            gw_part[r, :] = acc
        if not first:
            for k in range(BLK // 128):
                rows = slice(m * BLK + k * 128, m * BLK + (k + 1) * 128)
                dst = pl.ds(mo(h0 + m * BLK + k * 128, 128), 128)
                gw2[:, dst] = jnp.sum(jnp.transpose(gw_part[rows, :]), axis=0, keepdims=True)

    cp_q_own.wait_recv()
    mass_p, dq_p = penalty(q_far_sc[...] + rx_q_own[...], 1)

    for m in range(nb):
        weight_part(m, 1, True)
        readout_part(m, dq_p, 1, True)
    cp_q_far.wait_recv()
    mass_own, dq_own = penalty(q_own_sc[...] + rx_q_far[...], 0)
    for m in range(nb):
        if m < 2:
            weight_part(m, 0, False)
        readout_part(m, dq_own, 0, False)
    gw_at = pl.ds(h0, HH)
    cp_gw = far(gw2.at[:, gw_at], gw2.at[:, gw_at], pair_s.at[6], pair_r.at[6], partner)
    cp_gw.start()
    for m in range(2, nb):
        weight_part(m, 0, False)

    cp_q.wait_recv()
    lane = iota((8, 128), 1)
    left = lane < S

    def both(own, other):
        return jnp.where(left, own, other)

    floor_own, floor_p = jnp.minimum(xr[0, 8:9, :], xr[2, 8:9, :]), jnp.minimum(xr[1, 8:9, :], xr[3, 8:9, :])
    floor = both(pltpu.roll(row8(floor_own), 96, 1), row8(floor_p))
    q_data = both(row8(tx_q[...]), pltpu.roll(row8(rx_q[...]), 32, 1))
    rew = both(row8(tx_small[A + 1 : A + 2, :]), pltpu.roll(row8(rx_small[A + 1 : A + 2, :]), 32, 1))
    logp = both(row8(tx_small[A + 2 : A + 3, :]), pltpu.roll(row8(rx_small[A + 2 : A + 3, :]), 32, 1))
    target = rew + discount * (floor - entropy_temp * logp)
    td_gap = q_data - target
    gap_terms = td_gap * td_gap
    mass_terms = both(mass_own, mass_p) - q_data
    dq_data = ((2.0 * td_gap - penalty_weight) * (1.0 / COUNT))[0:1]
    dq_out[...] = jnp.transpose(jnp.broadcast_to(dq_data, (128, 128)))[0:COUNT]

    ag_all.wait_recv()
    unit = units[...]
    got_sum = spread[...].astype(f32)
    own_rows = [got_sum[16 * r : 16 * r + 8] for r in range(4)]
    other_rows = [got_sum[16 * r + 8 : 16 * r + 16] for r in range(4)]
    rest = jnp.concatenate(own_rows + other_rows, axis=0) - unit
    div_row = jnp.sum(unit * rest, axis=-1, keepdims=True)
    scale = 2.0 * diversity_weight / (COUNT - 1) / COUNT
    norms = jnp.concatenate([norm_own, norm_p], axis=0)
    dgrad = ((scale * rest - unit * (scale * div_row)) / norms).astype(bf16)
    rt[COUNT : 2 * COUNT, :] = dgrad
    tail_x[0:COUNT, :] = dgrad

    def total(row):
        return jnp.sum(jnp.where(lane < COUNT, row, 0.0)[0:1], axis=1, keepdims=True)

    div_sum = jnp.sum(div_row, axis=0, keepdims=True)
    first = lane[0:1]
    stats = jnp.where(first == 0, total(gap_terms), jnp.where(first == 1, total(mass_terms), div_sum))
    stats_out[...] = stats * (1.0 / COUNT)

    rs_all.wait_send()
    ag_all.wait_send()
    for c in x_copies + [cp_obs, cp_small, cp_g, cp_q, cp_q_own, cp_q_far]:
        c.wait_send()
    cp_gw.wait()
    return None


def run_main(*args):
    vm, dma = pltpu.VMEM, pltpu.SemaphoreType.DMA
    outs = [
        vm((HH, D), f32), vm((H, D), bf16), vm((2 * COUNT, D), bf16), vm((COUNT + S, D), bf16), vm((S, H), f32),
        vm((1, H), f32), vm((1, H), f32), vm((COUNT, 128), f32), vm((1, 128), f32),
    ]
    scratch = [
        vm((NACT, D), bf16), vm((NACT, D), bf16), vm((NACT, D), bf16),
        vm((3, 1, S), jnp.int32), vm((A, S), jnp.int32), vm((2, 1, S), f32),
        vm((2 * S, D), bf16), vm((2 * ROWS, D), bf16), vm((2 * S, D), bf16),
        vm((S, D), bf16), vm((S, D), bf16), vm((24, 128), f32), vm((24, 128), f32),
        vm((HH, 128), f32), vm((2, S, CH), f32), vm((S, D), f32), vm((S, D), f32), vm((1, 128), f32), vm((1, 128), f32),
        vm((COUNT, D), f32), vm((PLANE, 16, 128), bf16), vm((PLANE, 16, 128), bf16),
        vm((4, 9, 128), f32), vm((16, 128), bf16), vm((COUNT, D), bf16),
        vm((HH // BLK, BLK, ROWS), f32), vm((HH, 2 * ROWS), bf16), vm((HH, 2 * ROWS), bf16),
        vm((4, 128), f32), vm((4, 128), f32), vm((4, 128), f32), vm((4, 128), f32),
        vm((2 * ROWS, D), bf16), vm((HH, 128), f32),
        dma((10,)), dma((NCH,)), dma((7,)), dma((7,)),
        dma((3,)), dma((3,)), dma((4,)),
    ]
    return pl.pallas_call(
        main_kernel,
        out_shape=outs,
        in_specs=[pl.BlockSpec(memory_space=pltpu.HBM)] * len(args),
        out_specs=[pl.BlockSpec(memory_space=pltpu.VMEM)] * len(outs),
        scratch_shapes=scratch,
        compiler_params=pltpu.CompilerParams(collective_id=0, has_side_effects=True, vmem_limit_bytes=36 << 20),
        name="critics",
    )(*(pltpu.with_memory_space_constraint(a, pltpu.HBM) for a in args))


STEP = 256


def weight_kernel(
    part, w, rt, tail_x, ho, v, gw_in, dq_in, stats_in, out, gw2, stats, buf, lt, gw_sc, stats_sc, sems
):
    b = lax.axis_index("batch")
    stats_sc[...] = stats_in[:, 0:3]
    copies = [pltpu.make_async_copy(stats_sc, stats, sems.at[0])]
    copies[0].start()
    dq = jnp.concatenate([dq_in[...]] * (STEP // 128), axis=1)

    def terms(at):
        r = dot(tail_x[...], w[at, :], NT)
        h = jnp.concatenate([ho[:, at], r[COUNT : COUNT + S]], axis=0)
        dc = r[0:COUNT]
        th = jnp.tanh(h)
        p = 1.0 + th
        so = h * p
        slope = 0.5 * (p + so * (1.0 - th))
        gw_sc[:, at] = gw_in[:, at] + jnp.sum(dq * so + dc * slope, axis=0, keepdims=True)
        return h, th, p, slope, dc

    def near(m):
        return pl.ds(mo(b * HH + m * STEP, STEP), STEP)

    def back(m, h, th, p, slope, dc):
        vr = v[:, near(m)]
        curve = 0.5 * (p * (1.0 - th)) * (1.0 - h * th)
        lt[0:COUNT, m * STEP : (m + 1) * STEP] = (vr * (dq * slope + dc * curve)).astype(bf16)
        lt[COUNT : 2 * COUNT, m * STEP : (m + 1) * STEP] = (vr * slope).astype(bf16)

    last = HH // STEP
    own_next = {0: [1], 1: [2], 2: [3], 3: [4, 5], 4: [6, 7]}
    other_next = {4: [0, 1], 5: [2, 3, 4, 5, 6, 7]}
    back(0, *terms(near(0)))
    for m in range(last):
        r = slice(m * STEP, (m + 1) * STEP)
        buf[r, :] = part[r, :] + dot(lt[:, r], rt[...], TN)
        for k in own_next.get(m, []):
            back(k, *terms(near(k)))
        c = pltpu.make_async_copy(buf.at[pl.ds(m * STEP, STEP)], out.at[0, pl.ds(m * STEP, STEP)], sems.at[2 + m])
        c.start()
        copies.append(c)
        for k in other_next.get(m, []):
            terms(pl.ds(mo((1 - b) * HH + k * STEP, STEP), STEP))
        if m == 5:
            copies.append(pltpu.make_async_copy(gw_sc, gw2, sems.at[1]))
            copies[-1].start()
    for c in copies:
        c.wait()
    return None


def run_weight(*args):
    sds = jax.ShapeDtypeStruct
    hbm = pl.BlockSpec(memory_space=pltpu.HBM)
    vm = pltpu.VMEM
    return pl.pallas_call(
        weight_kernel,
        out_shape=[sds((1, HH, D), f32), sds((1, H), f32), sds((1, 3), f32)],
        in_specs=[pl.BlockSpec(memory_space=vm)] * len(args),
        out_specs=[hbm] * 3,
        scratch_shapes=[
            vm((HH, D), f32), vm((2 * COUNT, HH), bf16), vm((1, H), f32), vm((1, 3), f32),
            pltpu.SemaphoreType.DMA((2 + HH // STEP,)),
        ],
        compiler_params=pltpu.CompilerParams(vmem_limit_bytes=20 << 20),
        name="weights",
    )(*args)


def body(
    replay_obs, replay_next, batch_rows, data_action, next_action, sampled_actions,
    reward, next_logp, action_table, w1, w2,
):
    row = lambda x: x.reshape(1, S)
    parts = run_main(
        replay_obs, replay_next, row(batch_rows), row(data_action), row(next_action), sampled_actions.T,
        row(reward), row(next_logp), action_table, w1.reshape(H, D), w2,
    )
    return run_weight(*parts)


def solution(mesh):
    finer = Mesh(mesh.devices.reshape(4, 4, 2, 2, mesh.shape["batch"]), (*ENS, "batch"))
    placed = (
        P("batch", None), P("batch", None), P("batch"), P("batch"), P("batch"), P("batch", None),
        P("batch"), P("batch"), P(), P(ENS, None, None), P(ENS, None),
    )
    return jax.shard_map(
        body,
        mesh=finer,
        in_specs=placed,
        out_specs=(P(ENS, "batch", None), P(ENS, None), P(ENS, None)),
        check_vma=False,
    )
```

```python
import jax
import jax.numpy as jnp
from jax import lax
from jax.experimental import pallas as pl
from jax.experimental.pallas import tpu as pltpu
from jax.sharding import Mesh
from jax.sharding import PartitionSpec as P

ENS = ("ens_0", "ens_1", "ens_2", "ens_3")
MESH_ID = pl.DeviceIdType.MESH
f32, bf16 = jnp.float32, jnp.bfloat16

D, H, HH = 1024, 4096, 2048
S, A, NACT = 32, 16, 256
ROWS = S * A
CH = 512
NCH = H // CH
BLK = 512
SUB = 32
PLANE = 32
COUNT = 64
discount, entropy_temp, penalty_weight, diversity_weight = 0.99, 0.2, 1.0, 1000.0

NN = (((1,), (0,)), ((), ()))
NT = (((1,), (1,)), ((), ()))
TN = (((0,), (0,)), ((), ()))


def dot(a, b, dims=NN):
    return lax.dot_general(a, b, dims, preferred_element_type=f32)


def mo(x, m):
    return pl.multiple_of(x, m)


def each(lo, hi, fn):
    def step(k, carry):
        fn(k)
        return carry

    lax.fori_loop(lo, hi, step, 0)


def iota(shape, dim):
    return lax.broadcasted_iota(jnp.int32, shape, dim)


def row8(x):
    return jnp.broadcast_to(x, (8, 128))


def main_kernel(
    obs_hbm, next_hbm, rows_hbm, dact_hbm, nact_hbm, sact_hbm, rew_hbm, logp_hbm, table_hbm, w_hbm, v_hbm,
    part, wt, rt, tail_x, ho, v, gw2, dq_out, stats_out,
    w, tab_obs, tab_next, table, ids, sact, rl,
    xdn, xs, xd, tx_obs, rx_obs, tx_small, rx_small,
    vcol, h_next, gin, rx_g, tx_q, rx_q, units, rs_tx, rs_buf, xr, ag_tx, spread,
    h_buf, sl, silu, q_own_sc, q_far_sc, rx_q_own, rx_q_far, x_out, gw_part,
    in_sem, w_sem, pair_s, pair_r, x_s, x_r, many,
):
    z, y, xh, core = (lax.axis_index(n) for n in ENS)
    b = lax.axis_index("batch")
    me = z * 8 + y * 2 + core
    xpos = xh * 2 + b

    zs = [lax.rem(z + d, 4) for d in range(4)]
    ys = [lax.rem(y + d, 4) for d in range(4)]
    cores = [core, 1 - core]
    order = sorted(range(1, PLANE), key=lambda k: -((0, 1, 2, 1)[k // 8] + (0, 1, 2, 1)[k // 2 % 4]))

    def plane(k):
        pz, py, pc = zs[k // 8], ys[k // 2 % 4], cores[k % 2]
        return pz * 8 + py * 2 + pc, (pz, py, xh, pc, b)

    def line(d):
        p = lax.rem(xpos + d, 4)
        return (z, y, lax.div(p, 2), core, lax.rem(p, 2))

    partner = (z, y, xh, core, 1 - b)
    h0 = mo(b * HH, HH)

    def far(src, dst, ssem, rsem, device):
        return pltpu.make_async_remote_copy(
            src_ref=src, dst_ref=dst, send_sem=ssem, recv_sem=rsem, device_id=device, device_id_type=MESH_ID
        )

    loads = [
        pltpu.make_async_copy(src, dst, in_sem.at[i])
        for i, (src, dst) in enumerate(
            [
                (rows_hbm, ids.at[0]), (dact_hbm, ids.at[1]), (nact_hbm, ids.at[2]), (sact_hbm, sact),
                (rew_hbm, rl.at[0]), (logp_hbm, rl.at[1]),
                (obs_hbm, tab_obs), (table_hbm, table), (next_hbm, tab_next), (v_hbm, v),
            ]
        )
    ]
    for c in loads:
        c.start()

    def w_copy(c):
        at = pl.ds(c * CH, CH)
        return pltpu.make_async_copy(w_hbm.at[at], w.at[at], w_sem.at[c])

    barrier = pltpu.get_barrier_semaphore()

    def greet(device):
        pl.semaphore_signal(barrier, inc=1, device_id=device, device_id_type=MESH_ID)

    for k in order:
        greet(plane(k)[1])
    for d in (1, 2, 3):
        greet(line(d))
    for c in range(4):
        w_copy(c).start()

    for c in loads[:6]:
        c.wait()

    lanes = iota((S, NACT), 1).astype(f32)
    eye = iota((S, S), 0) == iota((S, S), 1)
    ones = jnp.ones((S, NACT), bf16)

    def one_hot(row, value):
        diag = jnp.where(eye, jnp.broadcast_to(row, (S, S)), 0.0).astype(bf16)
        return jnp.where(dot(diag, ones) == lanes, value, 0.0).astype(bf16)

    def sample_hot(sact_f):
        pick = jnp.where((iota((ROWS, S), 0) & (S - 1)) == iota((ROWS, S), 1), 1.0, 0.0).astype(bf16)
        each_sample = dot(pick, sact_f.astype(bf16), NT)
        mine = lax.shift_right_logical(iota((ROWS, A), 0), 5) == iota((ROWS, A), 1)
        index = dot(jnp.where(mine, each_sample, 0.0).astype(bf16), jnp.ones((A, NACT), bf16))
        return jnp.where(index == iota((ROWS, NACT), 1).astype(f32), 0.5, 0.0).astype(bf16)

    rows_oh, dact_oh, nact_oh = (one_hot(ids[i].astype(f32), 0.5) for i in range(3))
    own_hot = sample_hot(sact[...].astype(f32))
    tx_small[...] = jnp.zeros_like(tx_small)
    tx_small[0:A, 0:S] = sact[...].astype(f32)
    tx_small[A : A + 1, 0:S] = ids[1].astype(f32)
    tx_small[A + 1 : A + 2, 0:S] = rl[0]
    tx_small[A + 2 : A + 3, 0:S] = rl[1]
    for c in loads[6:]:
        c.wait()
    for c in range(4, NCH):
        w_copy(c).start()

    obs = dot(rows_oh, tab_obs[...])
    nxt = dot(rows_oh, tab_next[...])
    tx_obs[...] = obs.astype(bf16)
    half_data = (obs + dot(dact_oh, table[...])).astype(bf16)
    xdn[0:S, :] = half_data
    xdn[S : 2 * S, :] = (nxt + dot(nact_oh, table[...])).astype(bf16)
    xd[0:S, :] = half_data

    def own_act(c, q_acc):
        at = slice(c * CH, (c + 1) * CH)
        h = jnp.concatenate([ho[:, at], h_next[c % 2]], axis=0)
        th = jnp.tanh(h)
        p = 1.0 + th
        so = h * p
        vr = v[:, at]
        sv = so * vr
        for k in range(CH // 128):
            q_acc = q_acc + sv[:, k * 128 : (k + 1) * 128]
        co = (0.5 * vr * (p[0:S] + so[0:S] * (1.0 - th[0:S]))).astype(bf16)
        g = dot(co, w[at, :])
        gin[...] = g if c == 0 else gin[...] + g
        return q_acc

    def spread_v(i):
        at = pl.ds(mo(h0 + i * 128, 128), 128)
        vcol[i * 128 : (i + 1) * 128, :] = jnp.transpose(jnp.broadcast_to(0.5 * v[:, at], (128, 128)))

    q_acc = jnp.zeros((2 * S, 128), f32)
    cp_obs = far(tx_obs, rx_obs, pair_s.at[0], pair_r.at[0], partner)
    cp_small = far(tx_small, rx_small, pair_s.at[1], pair_r.at[1], partner)
    for c in range(NCH):
        if c % 2 == 0:
            w_copy(c).wait()
            w_copy(c + 1).wait()
        h = dot(xdn[...], w[c * CH : (c + 1) * CH, :], NT)
        ho[:, c * CH : (c + 1) * CH] = h[0:S]
        h_next[c % 2] = h[S : 2 * S]
        if c > 0:
            q_acc = own_act(c - 1, q_acc)
        for i in range(2):
            spread_v(2 * c + i)
    q_acc = own_act(NCH - 1, q_acc)
    q_own = jnp.sum(jnp.transpose(jnp.concatenate([q_acc, jnp.zeros((64, 128), f32)], axis=0)), axis=0, keepdims=True)
    tx_q[...] = q_own

    def norm_of(g):
        return jnp.sqrt(jnp.sum(g * g, axis=-1, keepdims=True) + 1.0)

    g_own = gin[...]
    norm_own = norm_of(g_own)
    u_own = g_own / norm_own
    units[0:S, :] = u_own
    q_hi = q_own.astype(bf16).astype(f32)
    q_mid = (q_own - q_hi).astype(bf16).astype(f32)
    q_rows = jnp.concatenate([q_hi, q_mid, q_own - q_hi - q_mid, jnp.zeros((5, 128), f32)], axis=0)
    for j in range(PLANE):
        r, c = j // 8, j % 8
        u_tile = u_own[8 * r : 8 * r + 8, 128 * c : 128 * c + 128]
        rs_tx[j] = jnp.concatenate([u_tile, q_rows], axis=0).astype(bf16)

    def rs_copy(k):
        j, device = plane(k)
        return far(rs_tx.at[j], rs_buf.at[k], many.at[0], many.at[1], device)

    all_in = rs_buf.at[pl.ds(1, PLANE - 1)]
    rs_all = far(all_in, all_in, many.at[0], many.at[1], partner)
    pl.semaphore_wait(barrier, PLANE - 1 + 3)
    for k in order:
        rs_copy(k).start()
    cp_obs.start()
    cp_small.start()
    cp_g = far(gin, rx_g, pair_s.at[2], pair_r.at[2], partner)
    cp_q = far(tx_q, rx_q, pair_s.at[3], pair_r.at[3], partner)
    cp_g.start()
    cp_q.start()

    def build(hot, base, off):
        for p in range(2):
            h_buf[p] = dot(hot, table[:, p * 512 : (p + 1) * 512])
        for i in range(A):
            for p in range(2):
                x = (base[:, p * 512 : (p + 1) * 512] + h_buf[p, i * S : (i + 1) * S, :]).astype(bf16)
                xs[off + i * S : off + (i + 1) * S, p * 512 : (p + 1) * 512] = x

    nb = HH // BLK

    def product(n):
        half, m = divmod(n, nb)
        h_buf[m] = dot(w[pl.ds(mo(h0 + m * BLK, BLK), BLK), :], xs[half * ROWS : (half + 1) * ROWS, :], NT)

    def activate(n, q):
        half, m = divmod(n, nb)
        at = slice(half * ROWS, (half + 1) * ROWS)
        for i in range(BLK // SUB):
            h = h_buf[m, i * SUB : (i + 1) * SUB, :]
            r = slice(m * BLK + i * SUB, m * BLK + (i + 1) * SUB)
            th = jnp.tanh(h)
            p = 1.0 + th
            so = h * p
            vh = vcol[r, :]
            vh = jnp.concatenate([vh, vh, vh, vh], axis=1)
            silu[r, at] = so.astype(bf16)
            sl[r, at] = (vh * (p + so * (1.0 - th))).astype(bf16)
            sv = so * vh
            q = q + ((sv[0:8] + sv[8:16]) + (sv[16:24] + sv[24:32]))
        return q

    def keep_q(q, ref):
        q = 2.0 * jnp.sum(q, axis=0, keepdims=True)
        for k in range(4):
            ref[k : k + 1, :] = q[:, k * 128 : (k + 1) * 128]

    q_zero = jnp.zeros((8, ROWS), f32)
    cp_q_own = far(q_own_sc, rx_q_own, pair_s.at[4], pair_r.at[4], partner)
    cp_q_far = far(q_far_sc, rx_q_far, pair_s.at[5], pair_r.at[5], partner)
    x_copies = [far(xr.at[0], xr.at[d], x_s.at[d - 1], x_r.at[d - 1], line(d)) for d in (1, 2, 3)]

    build(own_hot, obs, 0)
    product(0)
    q = q_zero
    for n in range(1, nb):
        product(n)
        q = activate(n - 1, q)

    cp_obs.wait_recv()
    cp_small.wait_recv()
    obs_p = rx_obs[...].astype(f32)
    build(sample_hot(rx_small[0:A, 0:S]), obs_p, ROWS)
    half_p = (obs_p + dot(one_hot(rx_small[A : A + 1, 0:S], 0.5), table[...])).astype(bf16)
    xd[S : 2 * S, :] = half_p
    tail_x[COUNT : COUNT + S, :] = half_p
    product(nb)
    keep_q(activate(nb - 1, q), q_own_sc)

    rs_all.wait_recv()
    rs_buf[0] = rs_tx[me]
    got = rs_buf[...].astype(f32)
    xr[0, 0:8, :] = jnp.sum(got[:, 0:8, :], axis=0)
    xr[0, 8:9, :] = jnp.min((got[:, 8:9, :] + got[:, 9:10, :]) + got[:, 10:11, :], axis=0)
    for c in x_copies:
        c.start()
    cp_q_own.start()
    q = q_zero
    for n in range(nb + 1, 2 * nb):
        product(n)
        q = activate(n - 1, q)

    keep_q(activate(2 * nb - 1, q), q_far_sc)
    cp_q_far.start()

    for c in x_copies:
        c.wait_recv()
    row_me = mo(lax.div(me, 8) * 16, 16)
    col_me = mo(lax.rem(me, 8) * 128, 128)
    ag_tx[...] = jnp.concatenate([xr[0, 0:8, :] + xr[2, 0:8, :], xr[1, 0:8, :] + xr[3, 0:8, :]], axis=0).astype(bf16)

    def ag_copy(k):
        dst = spread.at[pl.ds(row_me, 16), pl.ds(col_me, 128)]
        return far(ag_tx, dst, many.at[2], many.at[3], plane(k)[1])

    ag_all = far(all_in, all_in, many.at[2], many.at[3], partner)

    for k in order:
        ag_copy(k).start()
    spread[pl.ds(row_me, 16), pl.ds(col_me, 128)] = ag_tx[...]

    cp_g.wait_recv()
    g_p = rx_g[...]
    norm_p = norm_of(g_p)
    units[S : 2 * S, :] = g_p / norm_p
    rt[0:COUNT, :] = (xd[...].astype(f32) * 2.0).astype(bf16)

    def penalty(q4, half):
        m = row8(jnp.sum(jnp.exp(q4), axis=0, keepdims=True))
        m = m + pltpu.roll(m, 32, 1)
        mass = jnp.log(m + pltpu.roll(m, 64, 1))
        dq = jnp.exp(q4 - mass[0:4]) * (penalty_weight / COUNT)
        for r in range(4):
            col = jnp.transpose(jnp.broadcast_to(dq[r : r + 1, :], (128, 128))) * 2.0
            rows = slice(half * ROWS + r * 128, half * ROWS + (r + 1) * 128)
            for c in range(8):
                at = slice(c * 128, (c + 1) * 128)
                x_out[rows, at] = (xs[rows, at].astype(f32) * col).astype(bf16)
        return mass, dq

    def weight_part(m, half, first):
        at = slice(half * ROWS, (half + 1) * ROWS)
        r = slice(m * BLK, (m + 1) * BLK)
        g = dot(sl[r, at], x_out[at, :])
        part[r, :] = g if first else part[r, :] + g
        r = slice((half * nb + m) * BLK, (half * nb + m + 1) * BLK)
        wt[:, r] = jnp.transpose(w[r, :])

    def readout_part(m, dq, half, first):
        for i in range(BLK // SUB):
            r = slice(m * BLK + i * SUB, m * BLK + (i + 1) * SUB)
            acc = None if first else gw_part[r, :]
            for k in range(4):
                c = slice(half * ROWS + k * 128, half * ROWS + (k + 1) * 128)
                term = silu[r, c].astype(f32) * dq[k : k + 1, :]
                acc = term if acc is None else acc + term
            gw_part[r, :] = acc
        if not first:
            for k in range(BLK // 128):
                rows = slice(m * BLK + k * 128, m * BLK + (k + 1) * 128)
                dst = pl.ds(mo(h0 + m * BLK + k * 128, 128), 128)
                gw2[:, dst] = jnp.sum(jnp.transpose(gw_part[rows, :]), axis=0, keepdims=True)

    cp_q_own.wait_recv()
    mass_p, dq_p = penalty(q_far_sc[...] + rx_q_own[...], 1)

    for m in range(nb):
        weight_part(m, 1, True)
        readout_part(m, dq_p, 1, True)
    cp_q_far.wait_recv()
    mass_own, dq_own = penalty(q_own_sc[...] + rx_q_far[...], 0)
    for m in range(nb):
        if m < 2:
            weight_part(m, 0, False)
        readout_part(m, dq_own, 0, False)
    gw_at = pl.ds(h0, HH)
    cp_gw = far(gw2.at[:, gw_at], gw2.at[:, gw_at], pair_s.at[6], pair_r.at[6], partner)
    cp_gw.start()
    for m in range(2, nb):
        weight_part(m, 0, False)

    cp_q.wait_recv()
    lane = iota((8, 128), 1)
    left = lane < S

    def both(own, other):
        return jnp.where(left, own, other)

    floor_own, floor_p = jnp.minimum(xr[0, 8:9, :], xr[2, 8:9, :]), jnp.minimum(xr[1, 8:9, :], xr[3, 8:9, :])
    floor = both(pltpu.roll(row8(floor_own), 96, 1), row8(floor_p))
    q_data = both(row8(tx_q[...]), pltpu.roll(row8(rx_q[...]), 32, 1))
    rew = both(row8(tx_small[A + 1 : A + 2, :]), pltpu.roll(row8(rx_small[A + 1 : A + 2, :]), 32, 1))
    logp = both(row8(tx_small[A + 2 : A + 3, :]), pltpu.roll(row8(rx_small[A + 2 : A + 3, :]), 32, 1))
    target = rew + discount * (floor - entropy_temp * logp)
    td_gap = q_data - target
    gap_terms = td_gap * td_gap
    mass_terms = both(mass_own, mass_p) - q_data
    dq_data = ((2.0 * td_gap - penalty_weight) * (1.0 / COUNT))[0:1]
    dq_out[...] = jnp.transpose(jnp.broadcast_to(dq_data, (128, 128)))[0:COUNT]

    ag_all.wait_recv()
    unit = units[...]
    got_sum = spread[...].astype(f32)
    own_rows = [got_sum[16 * r : 16 * r + 8] for r in range(4)]
    other_rows = [got_sum[16 * r + 8 : 16 * r + 16] for r in range(4)]
    rest = jnp.concatenate(own_rows + other_rows, axis=0) - unit
    div_row = jnp.sum(unit * rest, axis=-1, keepdims=True)
    scale = 2.0 * diversity_weight / (COUNT - 1) / COUNT
    norms = jnp.concatenate([norm_own, norm_p], axis=0)
    dgrad = ((scale * rest - unit * (scale * div_row)) / norms).astype(bf16)
    rt[COUNT : 2 * COUNT, :] = dgrad
    tail_x[0:COUNT, :] = dgrad

    def total(row):
        return jnp.sum(jnp.where(lane < COUNT, row, 0.0)[0:1], axis=1, keepdims=True)

    div_sum = jnp.sum(div_row, axis=0, keepdims=True)
    first = lane[0:1]
    stats = jnp.where(first == 0, total(gap_terms), jnp.where(first == 1, total(mass_terms), div_sum))
    stats_out[...] = stats * (1.0 / COUNT)

    rs_all.wait_send()
    ag_all.wait_send()
    for c in x_copies + [cp_obs, cp_small, cp_g, cp_q, cp_q_own, cp_q_far]:
        c.wait_send()
    cp_gw.wait()
    return None


def run_main(*args):
    vm, dma = pltpu.VMEM, pltpu.SemaphoreType.DMA
    outs = [
        vm((HH, D), f32), vm((D, H), bf16), vm((2 * COUNT, D), bf16), vm((COUNT + S, D), bf16), vm((S, H), f32),
        vm((1, H), f32), vm((1, H), f32), vm((COUNT, 128), f32), vm((1, 128), f32),
    ]
    scratch = [
        vm((H, D), bf16), vm((NACT, D), bf16), vm((NACT, D), bf16), vm((NACT, D), bf16),
        vm((3, 1, S), jnp.int32), vm((A, S), jnp.int32), vm((2, 1, S), f32),
        vm((2 * S, D), bf16), vm((2 * ROWS, D), bf16), vm((2 * S, D), bf16),
        vm((S, D), bf16), vm((S, D), bf16), vm((24, 128), f32), vm((24, 128), f32),
        vm((HH, 128), f32), vm((2, S, CH), f32), vm((S, D), f32), vm((S, D), f32), vm((1, 128), f32), vm((1, 128), f32),
        vm((COUNT, D), f32), vm((PLANE, 16, 128), bf16), vm((PLANE, 16, 128), bf16),
        vm((4, 9, 128), f32), vm((16, 128), bf16), vm((COUNT, D), bf16),
        vm((HH // BLK, BLK, ROWS), f32), vm((HH, 2 * ROWS), bf16), vm((HH, 2 * ROWS), bf16),
        vm((4, 128), f32), vm((4, 128), f32), vm((4, 128), f32), vm((4, 128), f32),
        vm((2 * ROWS, D), bf16), vm((HH, 128), f32),
        dma((10,)), dma((NCH,)), dma((7,)), dma((7,)),
        dma((3,)), dma((3,)), dma((4,)),
    ]
    return pl.pallas_call(
        main_kernel,
        out_shape=outs,
        in_specs=[pl.BlockSpec(memory_space=pltpu.HBM)] * len(args),
        out_specs=[pl.BlockSpec(memory_space=pltpu.VMEM)] * len(outs),
        scratch_shapes=scratch,
        compiler_params=pltpu.CompilerParams(collective_id=0, has_side_effects=True, vmem_limit_bytes=36 << 20),
        name="critics",
    )(*(pltpu.with_memory_space_constraint(a, pltpu.HBM) for a in args))


def weight_kernel(
    part, wt, rt, tail_x, ho, v, gw_in, dq_in, stats_in, out, gw2, stats, buf, lt, gw_sc, stats_sc, sems
):
    b = lax.axis_index("batch")
    stats_sc[...] = stats_in[:, 0:3]
    copies = [pltpu.make_async_copy(stats_sc, stats, sems.at[0])]
    copies[0].start()

    def terms(start, size):
        at = pl.ds(mo(start, 256), size)
        dq = jnp.concatenate([dq_in[...]] * (size // 128), axis=1)
        r = dot(tail_x[...], wt[:, at])
        h = jnp.concatenate([ho[:, at], r[COUNT : COUNT + S]], axis=0)
        dc = r[0:COUNT]
        th = jnp.tanh(h)
        p = 1.0 + th
        so = h * p
        slope = 0.5 * (p + so * (1.0 - th))
        gw_sc[:, at] = gw_in[:, at] + jnp.sum(dq * so + dc * slope, axis=0, keepdims=True)
        return at, dq, h, th, p, slope, dc

    def back(start, size):
        at, dq, h, th, p, slope, dc = terms(b * HH + start, size)
        vr = v[:, at]
        curve = 0.5 * (p * (1.0 - th)) * (1.0 - h * th)
        lt[0:COUNT, start : start + size] = (vr * (dq * slope + dc * curve)).astype(bf16)
        lt[COUNT : 2 * COUNT, start : start + size] = (vr * slope).astype(bf16)

    blocks = ((0, 256), (256, 256), (512, 512), (1024, 512), (1536, 512))
    back(*blocks[0])
    for m, (start, size) in enumerate(blocks):
        r = slice(start, start + size)
        buf[r, :] = part[r, :] + dot(lt[:, r], rt[...], TN)
        if m + 1 < len(blocks):
            back(*blocks[m + 1])
        at = pl.ds(start, size)
        copies.append(pltpu.make_async_copy(buf.at[at], out.at[0, at], sems.at[2 + m]))
        copies[-1].start()
    for m in range(HH // BLK):
        terms((1 - b) * HH + m * BLK, BLK)
    copies.append(pltpu.make_async_copy(gw_sc, gw2, sems.at[1]))
    copies[-1].start()
    for c in copies:
        c.wait()
    return None


def run_weight(*args):
    sds = jax.ShapeDtypeStruct
    hbm = pl.BlockSpec(memory_space=pltpu.HBM)
    vm = pltpu.VMEM
    return pl.pallas_call(
        weight_kernel,
        out_shape=[sds((1, HH, D), f32), sds((1, H), f32), sds((1, 3), f32)],
        in_specs=[pl.BlockSpec(memory_space=vm)] * len(args),
        out_specs=[hbm] * 3,
        scratch_shapes=[
            vm((HH, D), f32), vm((2 * COUNT, HH), bf16), vm((1, H), f32), vm((1, 3), f32),
            pltpu.SemaphoreType.DMA((7,)),
        ],
        compiler_params=pltpu.CompilerParams(vmem_limit_bytes=20 << 20),
        name="weights",
    )(*args)


def body(
    replay_obs, replay_next, batch_rows, data_action, next_action, sampled_actions,
    reward, next_logp, action_table, w1, w2,
):
    row = lambda x: x.reshape(1, S)
    parts = run_main(
        replay_obs, replay_next, row(batch_rows), row(data_action), row(next_action), sampled_actions.T,
        row(reward), row(next_logp), action_table, w1.reshape(H, D), w2,
    )
    return run_weight(*parts)


def solution(mesh):
    finer = Mesh(mesh.devices.reshape(4, 4, 2, 2, mesh.shape["batch"]), (*ENS, "batch"))
    placed = (
        P("batch", None), P("batch", None), P("batch"), P("batch"), P("batch"), P("batch", None),
        P("batch"), P("batch"), P(), P(ENS, None, None), P(ENS, None),
    )
    return jax.shard_map(
        body,
        mesh=finer,
        in_specs=placed,
        out_specs=(P(ENS, "batch", None), P(ENS, None), P(ENS, None)),
        check_vma=False,
    )
```

```python
import jax
import jax.numpy as jnp
from jax import lax
from jax.experimental import pallas as pl
from jax.experimental.pallas import tpu as pltpu
from jax.sharding import Mesh
from jax.sharding import PartitionSpec as P

ENS = ("ens_0", "ens_1", "ens_2", "ens_3")
MESH_ID = pl.DeviceIdType.MESH
f32, bf16 = jnp.float32, jnp.bfloat16

D, H, HH = 1024, 4096, 2048
S, A, NACT = 32, 16, 256
ROWS = S * A
CH = 512
NCH = H // CH
BLK = 512
SUB = 32
PLANE = 32
COUNT = 64
discount, entropy_temp, penalty_weight, diversity_weight = 0.99, 0.2, 1.0, 1000.0

NN = (((1,), (0,)), ((), ()))
NT = (((1,), (1,)), ((), ()))
TN = (((0,), (0,)), ((), ()))


def dot(a, b, dims=NN):
    return lax.dot_general(a, b, dims, preferred_element_type=f32)


def mo(x, m):
    return pl.multiple_of(x, m)


def each(lo, hi, fn):
    def step(k, carry):
        fn(k)
        return carry

    lax.fori_loop(lo, hi, step, 0)


def iota(shape, dim):
    return lax.broadcasted_iota(jnp.int32, shape, dim)


def row8(x):
    return jnp.broadcast_to(x, (8, 128))


def main_kernel(
    obs_hbm, next_hbm, rows_hbm, dact_hbm, nact_hbm, sact_hbm, rew_hbm, logp_hbm, table_hbm, w_hbm, v_hbm,
    part, wt, rt, tail_x, ho, v, gw2, dq_out, stats_out,
    w, tab_obs, tab_next, table, ids, sact, rl,
    xdn, xs, xd, tx_obs, rx_obs, tx_small, rx_small,
    vcol, h_next, gin, rx_g, tx_q, rx_q, units, rs_tx, rs_buf, xr, ag_tx, spread,
    h_buf, sl, silu, q_own_sc, q_far_sc, rx_q_own, rx_q_far, x_out, gw_part,
    in_sem, w_sem, pair_s, pair_r, x_s, x_r, many,
):
    z, y, xh, core = (lax.axis_index(n) for n in ENS)
    b = lax.axis_index("batch")
    me = z * 8 + y * 2 + core
    xpos = xh * 2 + b

    zs = [lax.rem(z + d, 4) for d in range(4)]
    ys = [lax.rem(y + d, 4) for d in range(4)]
    cores = [core, 1 - core]
    order = sorted(range(1, PLANE), key=lambda k: -((0, 1, 2, 1)[k // 8] + (0, 1, 2, 1)[k // 2 % 4]))

    def plane(k):
        pz, py, pc = zs[k // 8], ys[k // 2 % 4], cores[k % 2]
        return pz * 8 + py * 2 + pc, (pz, py, xh, pc, b)

    def line(d):
        p = lax.rem(xpos + d, 4)
        return (z, y, lax.div(p, 2), core, lax.rem(p, 2))

    partner = (z, y, xh, core, 1 - b)
    h0 = mo(b * HH, HH)

    def far(src, dst, ssem, rsem, device):
        return pltpu.make_async_remote_copy(
            src_ref=src, dst_ref=dst, send_sem=ssem, recv_sem=rsem, device_id=device, device_id_type=MESH_ID
        )

    loads = [
        pltpu.make_async_copy(src, dst, in_sem.at[i])
        for i, (src, dst) in enumerate(
            [
                (rows_hbm, ids.at[0]), (dact_hbm, ids.at[1]), (nact_hbm, ids.at[2]), (sact_hbm, sact),
                (rew_hbm, rl.at[0]), (logp_hbm, rl.at[1]),
                (obs_hbm, tab_obs), (table_hbm, table), (next_hbm, tab_next), (v_hbm, v),
            ]
        )
    ]
    for c in loads:
        c.start()

    def w_copy(c):
        at = pl.ds(c * CH, CH)
        return pltpu.make_async_copy(w_hbm.at[at], w.at[at], w_sem.at[c])

    barrier = pltpu.get_barrier_semaphore()

    def greet(device):
        pl.semaphore_signal(barrier, inc=1, device_id=device, device_id_type=MESH_ID)

    for k in order:
        greet(plane(k)[1])
    for d in (1, 2, 3):
        greet(line(d))
    for c in range(4):
        w_copy(c).start()

    for c in loads[:6]:
        c.wait()

    lanes = iota((S, NACT), 1).astype(f32)
    eye = iota((S, S), 0) == iota((S, S), 1)
    ones = jnp.ones((S, NACT), bf16)

    def one_hot(row, value):
        diag = jnp.where(eye, jnp.broadcast_to(row, (S, S)), 0.0).astype(bf16)
        return jnp.where(dot(diag, ones) == lanes, value, 0.0).astype(bf16)

    def sample_hot(sact_f):
        pick = jnp.where((iota((ROWS, S), 0) & (S - 1)) == iota((ROWS, S), 1), 1.0, 0.0).astype(bf16)
        each_sample = dot(pick, sact_f.astype(bf16), NT)
        mine = lax.shift_right_logical(iota((ROWS, A), 0), 5) == iota((ROWS, A), 1)
        index = dot(jnp.where(mine, each_sample, 0.0).astype(bf16), jnp.ones((A, NACT), bf16))
        return jnp.where(index == iota((ROWS, NACT), 1).astype(f32), 0.5, 0.0).astype(bf16)

    rows_oh, dact_oh, nact_oh = (one_hot(ids[i].astype(f32), 0.5) for i in range(3))
    own_hot = sample_hot(sact[...].astype(f32))
    tx_small[...] = jnp.zeros_like(tx_small)
    tx_small[0:A, 0:S] = sact[...].astype(f32)
    tx_small[A : A + 1, 0:S] = ids[1].astype(f32)
    tx_small[A + 1 : A + 2, 0:S] = rl[0]
    tx_small[A + 2 : A + 3, 0:S] = rl[1]
    for c in loads[6:]:
        c.wait()
    for c in range(4, NCH):
        w_copy(c).start()

    obs = dot(rows_oh, tab_obs[...])
    nxt = dot(rows_oh, tab_next[...])
    tx_obs[...] = obs.astype(bf16)
    acts = dot(jnp.concatenate([dact_oh, nact_oh], axis=0), table[...])
    half_data = (obs + acts[0:S]).astype(bf16)
    xdn[0:S, :] = half_data
    xdn[S : 2 * S, :] = (nxt + acts[S : 2 * S]).astype(bf16)
    xd[0:S, :] = half_data

    def own_act(c, q_acc):
        at = slice(c * CH, (c + 1) * CH)
        h = jnp.concatenate([ho[:, at], h_next[c % 2]], axis=0)
        th = jnp.tanh(h)
        p = 1.0 + th
        so = h * p
        vr = v[:, at]
        sv = so * vr
        for k in range(CH // 128):
            q_acc = q_acc + sv[:, k * 128 : (k + 1) * 128]
        co = (0.5 * vr * (p[0:S] + so[0:S] * (1.0 - th[0:S]))).astype(bf16)
        g = dot(co, w[at, :])
        gin[...] = g if c == 0 else gin[...] + g
        return q_acc

    def spread_v(i):
        at = pl.ds(mo(h0 + i * 128, 128), 128)
        vcol[i * 128 : (i + 1) * 128, :] = jnp.transpose(jnp.broadcast_to(0.5 * v[:, at], (128, 128)))

    q_acc = jnp.zeros((2 * S, 128), f32)
    cp_obs = far(tx_obs, rx_obs, pair_s.at[0], pair_r.at[0], partner)
    cp_small = far(tx_small, rx_small, pair_s.at[1], pair_r.at[1], partner)
    for c in range(NCH):
        if c % 2 == 0:
            w_copy(c).wait()
            w_copy(c + 1).wait()
        h = dot(xdn[...], w[c * CH : (c + 1) * CH, :], NT)
        ho[:, c * CH : (c + 1) * CH] = h[0:S]
        h_next[c % 2] = h[S : 2 * S]
        if c > 0:
            q_acc = own_act(c - 1, q_acc)
        for i in range(2):
            spread_v(2 * c + i)
    q_acc = own_act(NCH - 1, q_acc)
    q_own = jnp.sum(jnp.transpose(jnp.concatenate([q_acc, jnp.zeros((64, 128), f32)], axis=0)), axis=0, keepdims=True)
    tx_q[...] = q_own

    def norm_of(g):
        return jnp.sqrt(jnp.sum(g * g, axis=-1, keepdims=True) + 1.0)

    g_own = gin[...]
    norm_own = norm_of(g_own)
    u_own = g_own / norm_own
    units[0:S, :] = u_own
    q_hi = q_own.astype(bf16).astype(f32)
    q_mid = (q_own - q_hi).astype(bf16).astype(f32)
    q_rows = jnp.concatenate([q_hi, q_mid, q_own - q_hi - q_mid, jnp.zeros((5, 128), f32)], axis=0)
    for j in range(PLANE):
        r, c = j // 8, j % 8
        u_tile = u_own[8 * r : 8 * r + 8, 128 * c : 128 * c + 128]
        rs_tx[j] = jnp.concatenate([u_tile, q_rows], axis=0).astype(bf16)

    def rs_copy(k):
        j, device = plane(k)
        return far(rs_tx.at[j], rs_buf.at[k], many.at[0], many.at[1], device)

    all_in = rs_buf.at[pl.ds(1, PLANE - 1)]
    rs_all = far(all_in, all_in, many.at[0], many.at[1], partner)
    pl.semaphore_wait(barrier, PLANE - 1 + 3)
    for k in order:
        rs_copy(k).start()
    cp_obs.start()
    cp_small.start()
    cp_g = far(gin, rx_g, pair_s.at[2], pair_r.at[2], partner)
    cp_q = far(tx_q, rx_q, pair_s.at[3], pair_r.at[3], partner)
    cp_g.start()
    cp_q.start()

    def build(hot, base, off):
        for p in range(2):
            h_buf[p] = dot(hot, table[:, p * 512 : (p + 1) * 512])
        for i in range(A):
            for p in range(2):
                x = (base[:, p * 512 : (p + 1) * 512] + h_buf[p, i * S : (i + 1) * S, :]).astype(bf16)
                xs[off + i * S : off + (i + 1) * S, p * 512 : (p + 1) * 512] = x

    nb = HH // BLK

    def product(n):
        half, m = divmod(n, nb)
        h_buf[m] = dot(w[pl.ds(mo(h0 + m * BLK, BLK), BLK), :], xs[half * ROWS : (half + 1) * ROWS, :], NT)

    def activate(n, q):
        half, m = divmod(n, nb)
        at = slice(half * ROWS, (half + 1) * ROWS)
        for i in range(BLK // SUB):
            h = h_buf[m, i * SUB : (i + 1) * SUB, :]
            r = slice(m * BLK + i * SUB, m * BLK + (i + 1) * SUB)
            th = jnp.tanh(h)
            p = 1.0 + th
            so = h * p
            vh = vcol[r, :]
            vh = jnp.concatenate([vh, vh, vh, vh], axis=1)
            silu[r, at] = so.astype(bf16)
            sl[r, at] = (vh * (p + so * (1.0 - th))).astype(bf16)
            sv = so * vh
            q = q + ((sv[0:8] + sv[8:16]) + (sv[16:24] + sv[24:32]))
        return q

    def keep_q(q, ref):
        q = 2.0 * jnp.sum(q, axis=0, keepdims=True)
        for k in range(4):
            ref[k : k + 1, :] = q[:, k * 128 : (k + 1) * 128]

    q_zero = jnp.zeros((8, ROWS), f32)
    cp_q_own = far(q_own_sc, rx_q_own, pair_s.at[4], pair_r.at[4], partner)
    cp_q_far = far(q_far_sc, rx_q_far, pair_s.at[5], pair_r.at[5], partner)
    x_copies = [far(xr.at[0], xr.at[d], x_s.at[d - 1], x_r.at[d - 1], line(d)) for d in (1, 2, 3)]

    build(own_hot, obs, 0)
    product(0)
    q = q_zero
    for n in range(1, nb):
        product(n)
        q = activate(n - 1, q)

    cp_obs.wait_recv()
    cp_small.wait_recv()
    obs_p = rx_obs[...].astype(f32)
    build(sample_hot(rx_small[0:A, 0:S]), obs_p, ROWS)
    half_p = (obs_p + dot(one_hot(rx_small[A : A + 1, 0:S], 0.5), table[...])).astype(bf16)
    xd[S : 2 * S, :] = half_p
    tail_x[COUNT : COUNT + S, :] = half_p
    product(nb)
    keep_q(activate(nb - 1, q), q_own_sc)

    rs_all.wait_recv()
    rs_buf[0] = rs_tx[me]
    got = rs_buf[...].astype(f32)
    xr[0, 0:8, :] = jnp.sum(got[:, 0:8, :], axis=0)
    xr[0, 8:9, :] = jnp.min((got[:, 8:9, :] + got[:, 9:10, :]) + got[:, 10:11, :], axis=0)
    for c in x_copies:
        c.start()
    cp_q_own.start()
    q = q_zero
    for n in range(nb + 1, 2 * nb):
        product(n)
        q = activate(n - 1, q)

    keep_q(activate(2 * nb - 1, q), q_far_sc)
    cp_q_far.start()

    for c in x_copies:
        c.wait_recv()
    row_me = mo(lax.div(me, 8) * 16, 16)
    col_me = mo(lax.rem(me, 8) * 128, 128)
    ag_tx[...] = jnp.concatenate([xr[0, 0:8, :] + xr[2, 0:8, :], xr[1, 0:8, :] + xr[3, 0:8, :]], axis=0).astype(bf16)

    def ag_copy(k):
        dst = spread.at[pl.ds(row_me, 16), pl.ds(col_me, 128)]
        return far(ag_tx, dst, many.at[2], many.at[3], plane(k)[1])

    ag_all = far(all_in, all_in, many.at[2], many.at[3], partner)

    for k in order:
        ag_copy(k).start()
    spread[pl.ds(row_me, 16), pl.ds(col_me, 128)] = ag_tx[...]

    cp_g.wait_recv()
    g_p = rx_g[...]
    norm_p = norm_of(g_p)
    units[S : 2 * S, :] = g_p / norm_p
    rt[0:COUNT, :] = (xd[...].astype(f32) * 2.0).astype(bf16)

    def penalty(q4, half):
        m = row8(jnp.sum(jnp.exp(q4), axis=0, keepdims=True))
        m = m + pltpu.roll(m, 32, 1)
        mass = jnp.log(m + pltpu.roll(m, 64, 1))
        dq = jnp.exp(q4 - mass[0:4]) * (penalty_weight / COUNT)
        for r in range(4):
            col = jnp.transpose(jnp.broadcast_to(dq[r : r + 1, :], (128, 128))) * 2.0
            rows = slice(half * ROWS + r * 128, half * ROWS + (r + 1) * 128)
            for c in range(8):
                at = slice(c * 128, (c + 1) * 128)
                x_out[rows, at] = (xs[rows, at].astype(f32) * col).astype(bf16)
        return mass, dq

    def weight_part(m, half, first):
        at = slice(half * ROWS, (half + 1) * ROWS)
        r = slice(m * BLK, (m + 1) * BLK)
        g = dot(sl[r, at], x_out[at, :])
        part[r, :] = g if first else part[r, :] + g
        r = slice((half * nb + m) * BLK, (half * nb + m + 1) * BLK)
        wt[:, r] = jnp.transpose(w[r, :])

    def readout_part(m, dq, half, first):
        for i in range(BLK // SUB):
            r = slice(m * BLK + i * SUB, m * BLK + (i + 1) * SUB)
            acc = None if first else gw_part[r, :]
            for k in range(4):
                c = slice(half * ROWS + k * 128, half * ROWS + (k + 1) * 128)
                term = silu[r, c].astype(f32) * dq[k : k + 1, :]
                acc = term if acc is None else acc + term
            gw_part[r, :] = acc
        if not first:
            for k in range(BLK // 128):
                rows = slice(m * BLK + k * 128, m * BLK + (k + 1) * 128)
                dst = pl.ds(mo(h0 + m * BLK + k * 128, 128), 128)
                gw2[:, dst] = jnp.sum(jnp.transpose(gw_part[rows, :]), axis=0, keepdims=True)

    cp_q_own.wait_recv()
    mass_p, dq_p = penalty(q_far_sc[...] + rx_q_own[...], 1)

    for m in range(nb):
        weight_part(m, 1, True)
        readout_part(m, dq_p, 1, True)
    cp_q_far.wait_recv()
    mass_own, dq_own = penalty(q_own_sc[...] + rx_q_far[...], 0)
    for m in range(nb):
        if m < 1:
            weight_part(m, 0, False)
        readout_part(m, dq_own, 0, False)
    gw_at = pl.ds(h0, HH)
    cp_gw = far(gw2.at[:, gw_at], gw2.at[:, gw_at], pair_s.at[6], pair_r.at[6], partner)
    cp_gw.start()
    for m in range(1, nb):
        weight_part(m, 0, False)

    cp_q.wait_recv()
    lane = iota((8, 128), 1)
    left = lane < S

    def both(own, other):
        return jnp.where(left, own, other)

    floor_own, floor_p = jnp.minimum(xr[0, 8:9, :], xr[2, 8:9, :]), jnp.minimum(xr[1, 8:9, :], xr[3, 8:9, :])
    floor = both(pltpu.roll(row8(floor_own), 96, 1), row8(floor_p))
    q_data = both(row8(tx_q[...]), pltpu.roll(row8(rx_q[...]), 32, 1))
    rew = both(row8(tx_small[A + 1 : A + 2, :]), pltpu.roll(row8(rx_small[A + 1 : A + 2, :]), 32, 1))
    logp = both(row8(tx_small[A + 2 : A + 3, :]), pltpu.roll(row8(rx_small[A + 2 : A + 3, :]), 32, 1))
    target = rew + discount * (floor - entropy_temp * logp)
    td_gap = q_data - target
    gap_terms = td_gap * td_gap
    mass_terms = both(mass_own, mass_p) - q_data
    dq_data = ((2.0 * td_gap - penalty_weight) * (1.0 / COUNT))[0:1]
    dq_out[...] = jnp.transpose(jnp.broadcast_to(dq_data, (128, 128)))[0:COUNT]

    ag_all.wait_recv()
    unit = units[...]
    got_sum = spread[...].astype(f32)
    own_rows = [got_sum[16 * r : 16 * r + 8] for r in range(4)]
    other_rows = [got_sum[16 * r + 8 : 16 * r + 16] for r in range(4)]
    rest = jnp.concatenate(own_rows + other_rows, axis=0) - unit
    div_row = jnp.sum(unit * rest, axis=-1, keepdims=True)
    scale = 2.0 * diversity_weight / (COUNT - 1) / COUNT
    norms = jnp.concatenate([norm_own, norm_p], axis=0)
    dgrad = ((scale * rest - unit * (scale * div_row)) / norms).astype(bf16)
    rt[COUNT : 2 * COUNT, :] = dgrad
    tail_x[0:COUNT, :] = dgrad

    def total(row):
        return jnp.sum(jnp.where(lane < COUNT, row, 0.0)[0:1], axis=1, keepdims=True)

    div_sum = jnp.sum(div_row, axis=0, keepdims=True)
    first = lane[0:1]
    stats = jnp.where(first == 0, total(gap_terms), jnp.where(first == 1, total(mass_terms), div_sum))
    stats_out[...] = stats * (1.0 / COUNT)

    rs_all.wait_send()
    ag_all.wait_send()
    for c in x_copies + [cp_obs, cp_small, cp_g, cp_q, cp_q_own, cp_q_far]:
        c.wait_send()
    cp_gw.wait()
    return None


def run_main(*args):
    vm, dma = pltpu.VMEM, pltpu.SemaphoreType.DMA
    outs = [
        vm((HH, D), f32), vm((D, H), bf16), vm((2 * COUNT, D), bf16), vm((COUNT + S, D), bf16), vm((S, H), f32),
        vm((1, H), f32), vm((1, H), f32), vm((COUNT, 128), f32), vm((1, 128), f32),
    ]
    scratch = [
        vm((H, D), bf16), vm((NACT, D), bf16), vm((NACT, D), bf16), vm((NACT, D), bf16),
        vm((3, 1, S), jnp.int32), vm((A, S), jnp.int32), vm((2, 1, S), f32),
        vm((2 * S, D), bf16), vm((2 * ROWS, D), bf16), vm((2 * S, D), bf16),
        vm((S, D), bf16), vm((S, D), bf16), vm((24, 128), f32), vm((24, 128), f32),
        vm((HH, 128), f32), vm((2, S, CH), f32), vm((S, D), f32), vm((S, D), f32), vm((1, 128), f32), vm((1, 128), f32),
        vm((COUNT, D), f32), vm((PLANE, 16, 128), bf16), vm((PLANE, 16, 128), bf16),
        vm((4, 9, 128), f32), vm((16, 128), bf16), vm((COUNT, D), bf16),
        vm((HH // BLK, BLK, ROWS), f32), vm((HH, 2 * ROWS), bf16), vm((HH, 2 * ROWS), bf16),
        vm((4, 128), f32), vm((4, 128), f32), vm((4, 128), f32), vm((4, 128), f32),
        vm((2 * ROWS, D), bf16), vm((HH, 128), f32),
        dma((10,)), dma((NCH,)), dma((7,)), dma((7,)),
        dma((3,)), dma((3,)), dma((4,)),
    ]
    return pl.pallas_call(
        main_kernel,
        out_shape=outs,
        in_specs=[pl.BlockSpec(memory_space=pltpu.HBM)] * len(args),
        out_specs=[pl.BlockSpec(memory_space=pltpu.VMEM)] * len(outs),
        scratch_shapes=scratch,
        compiler_params=pltpu.CompilerParams(collective_id=0, has_side_effects=True, vmem_limit_bytes=36 << 20),
        name="critics",
    )(*(pltpu.with_memory_space_constraint(a, pltpu.HBM) for a in args))


def weight_kernel(
    part, wt, rt, tail_x, ho, v, gw_in, dq_in, stats_in, out, gw2, stats, buf, lt, gw_sc, stats_sc, sems
):
    b = lax.axis_index("batch")
    stats_sc[...] = stats_in[:, 0:3]
    copies = [pltpu.make_async_copy(stats_sc, stats, sems.at[0])]
    copies[0].start()

    def terms(start, size):
        at = pl.ds(mo(start, 256), size)
        dq = jnp.concatenate([dq_in[...]] * (size // 128), axis=1)
        r = dot(tail_x[...], wt[:, at])
        h = jnp.concatenate([ho[:, at], r[COUNT : COUNT + S]], axis=0)
        dc = r[0:COUNT]
        th = jnp.tanh(h)
        p = 1.0 + th
        so = h * p
        slope = 0.5 * (p + so * (1.0 - th))
        gw_sc[:, at] = gw_in[:, at] + jnp.sum(dq * so + dc * slope, axis=0, keepdims=True)
        return at, dq, h, th, p, slope, dc

    def back(start, size):
        at, dq, h, th, p, slope, dc = terms(b * HH + start, size)
        vr = v[:, at]
        curve = 0.5 * (p * (1.0 - th)) * (1.0 - h * th)
        lt[0:COUNT, start : start + size] = (vr * (dq * slope + dc * curve)).astype(bf16)
        lt[COUNT : 2 * COUNT, start : start + size] = (vr * slope).astype(bf16)

    blocks = ((0, 256), (256, 256), (512, 512), (1024, 512), (1536, 512))
    back(*blocks[0])
    for m, (start, size) in enumerate(blocks):
        r = slice(start, start + size)
        buf[r, :] = part[r, :] + dot(lt[:, r], rt[...], TN)
        if m + 1 < len(blocks):
            back(*blocks[m + 1])
        at = pl.ds(start, size)
        copies.append(pltpu.make_async_copy(buf.at[at], out.at[0, at], sems.at[2 + m]))
        copies[-1].start()
    for m in range(HH // BLK):
        terms((1 - b) * HH + m * BLK, BLK)
    copies.append(pltpu.make_async_copy(gw_sc, gw2, sems.at[1]))
    copies[-1].start()
    for c in copies:
        c.wait()
    return None


def run_weight(*args):
    sds = jax.ShapeDtypeStruct
    hbm = pl.BlockSpec(memory_space=pltpu.HBM)
    vm = pltpu.VMEM
    return pl.pallas_call(
        weight_kernel,
        out_shape=[sds((1, HH, D), f32), sds((1, H), f32), sds((1, 3), f32)],
        in_specs=[pl.BlockSpec(memory_space=vm)] * len(args),
        out_specs=[hbm] * 3,
        scratch_shapes=[
            vm((HH, D), f32), vm((2 * COUNT, HH), bf16), vm((1, H), f32), vm((1, 3), f32),
            pltpu.SemaphoreType.DMA((7,)),
        ],
        compiler_params=pltpu.CompilerParams(vmem_limit_bytes=20 << 20),
        name="weights",
    )(*args)


def body(
    replay_obs, replay_next, batch_rows, data_action, next_action, sampled_actions,
    reward, next_logp, action_table, w1, w2,
):
    row = lambda x: x.reshape(1, S)
    parts = run_main(
        replay_obs, replay_next, row(batch_rows), row(data_action), row(next_action), sampled_actions.T,
        row(reward), row(next_logp), action_table, w1.reshape(H, D), w2,
    )
    return run_weight(*parts)


def solution(mesh):
    finer = Mesh(mesh.devices.reshape(4, 4, 2, 2, mesh.shape["batch"]), (*ENS, "batch"))
    placed = (
        P("batch", None), P("batch", None), P("batch"), P("batch"), P("batch"), P("batch", None),
        P("batch"), P("batch"), P(), P(ENS, None, None), P(ENS, None),
    )
    return jax.shard_map(
        body,
        mesh=finer,
        in_specs=placed,
        out_specs=(P(ENS, "batch", None), P(ENS, None), P(ENS, None)),
        check_vma=False,
    )
```
